256 devices in a mesh: cls: 64 (over x, z, y_lo), dp: 4 (over y_hi, core).
Axes of the slice: x: 4, y: 4 (y_hi: 2, y_lo: 2; y = y_hi * 2 + y_lo), z: 8, core: 2. Of those that a mesh axis runs over, the one named last changes fastest.
Arguments:
- embeddings: bfloat16 [2048, 512], P(('dp', 'cls')), parts along dimension 0, may hold values from -4.4194174 to 4.4194174
- labels: int32 [2048], P(('dp', 'cls')), parts along dimension 0, may hold values from 0 to 262143
- centers: bfloat16 [1048576, 512], P(('dp', 'cls')), parts along dimension 0, may hold values from -3.0935922 to 3.0935922
Outputs:
- losses: float32 [2048], P(('dp', 'cls')), parts along dimension 0
- emb_grad: float32 [2048, 512], P(('dp', 'cls')), parts along dimension 0
- center_grad: float32 [1048576, 512], P(('dp', 'cls')), parts along dimension 0
The draws below stay inside these ranges and needn't reach their ends.
There are 4 independent parts, one for each index of `dp`. The reference program is written for one: setup_inputs(seed, part) draws one part's arguments, and reference() takes and returns one part's arrays. A program takes and returns all parts, laid end to end along the dimension named above; each array names one. Nothing has to cross between parts.
All inputs are finite; a program needn't handle non-finite values.
Results may differ from the reference program's by a relative error of at most 0.0042.
Values may be sent and summed in bfloat16 or wider, within the bound.
A program may use at most 64 MiB of HBM per device.

```python
import math
import jax
import jax.numpy as jnp
from jax import lax

D = 512
C_DEV = 4096
CLASSES = 262144
BATCH = 512
N_CLS = 64


def shared_direction(key):
    return jnp.clip(jax.random.normal(jax.random.fold_in(key, 101), (D,), jnp.float32), -3.0, 3.0)


def noisy_rows(key, row_count):
    noise_key = jax.random.fold_in(key, 11)
    scale_key = jax.random.fold_in(key, 12)
    noise_part = jnp.clip(jax.random.normal(noise_key, (row_count, D), jnp.float32), -5.0, 5.0)
    scales = jnp.exp(jax.random.uniform(scale_key, (row_count, 1), jnp.float32, 0.0, math.log(10.0)))
    return (noise_part, scales)


def draw_embeddings(key, part):
    direction = shared_direction(key)
    noise_part, scales = noisy_rows(jax.random.fold_in(key, 21), BATCH)
    lean_share = 0.3
    values = scales * (noise_part + lean_share * direction[None, :]) / math.sqrt(D)
    return values.astype(jnp.bfloat16)


def draw_centers(key, part):
    direction = shared_direction(key)
    noise_part, scales = noisy_rows(jax.random.fold_in(key, 31), CLASSES)
    ramp_share = 0.06
    ramp = jnp.arange(CLASSES, dtype=jnp.float32) / max(CLASSES - 1, 1) * ramp_share
    values = scales * (noise_part + ramp[:, None] * direction[None, :]) / math.sqrt(D)
    return values.astype(jnp.bfloat16)


def place_ends(entries, key, least, high):
    longest = entries.shape.index(max(entries.shape))
    spots = []
    for shift in (0, 1):
        where = [jax.random.randint(jax.random.fold_in(key, axis), (), 0, length) for axis, length in enumerate(entries.shape)]
        where[longest] = (where[longest] + shift) % entries.shape[longest]
        spots.append(tuple(where))
    return entries.at[spots[0]].set(least).at[spots[1]].set(high)


def setup_inputs(seed: int = 0, part: int = 0) -> dict:
    streams_of = jax.random.split(jax.random.key(seed), 4)
    part_splits = jax.random.split(jax.random.fold_in(streams_of[3], part), 4)
    embeddings = draw_embeddings(jax.random.fold_in(jax.random.fold_in(streams_of[3], part), 71), part)
    labels = place_ends(jax.random.randint(part_splits[1], (BATCH,), 0, CLASSES), jax.random.fold_in(part_splits[1], 1), 0, CLASSES - 1).astype(jnp.int32)
    centers = draw_centers(jax.random.fold_in(jax.random.fold_in(streams_of[3], part), 71), part)
    return dict(embeddings=embeddings, labels=labels, centers=centers)


logit_scale = 64.0
margin_cosine = math.cos(0.5)
margin_sine = math.sin(0.5)
sine_soften = 0.04
norm_eps = 1e-06

def unit_rows(values):
    widened = values.astype(jnp.float32)
    inverse = lax.rsqrt(lax.optimization_barrier(jnp.sum(widened * widened, axis=1, keepdims=True)) + norm_eps)
    normed = widened * inverse
    return (inverse, normed, normed.astype(jnp.bfloat16))

def score_block(rows_hat, rows_label, center_block, class_base):
    cosine = jnp.dot(rows_hat, center_block.T, preferred_element_type=jnp.float32)
    local_col = rows_label - class_base
    is_owned = (local_col >= 0) & (local_col < center_block.shape[0])
    column = lax.broadcasted_iota(jnp.int32, cosine.shape, 1)
    target_mask = column == local_col[:, None]
    target_cos = lax.optimization_barrier(jnp.sum(jnp.where(target_mask, cosine, 0.0), axis=1))
    target_sine = jnp.sqrt(1.0 + sine_soften - target_cos * target_cos)
    shifted = target_cos * margin_cosine - target_sine * margin_sine
    slopes = margin_cosine + margin_sine * target_cos / target_sine
    logits = jnp.where(target_mask, logit_scale * shifted[:, None], logit_scale * cosine)
    exp_terms = jnp.exp(logits - logit_scale)
    row_total = lax.optimization_barrier(jnp.sum(exp_terms, axis=1))
    weighted = (logit_scale * exp_terms * jnp.where(target_mask, slopes[:, None], 1.0)).astype(jnp.bfloat16)
    target = jnp.where(is_owned, logit_scale * shifted, 0.0)
    columns = jnp.where(is_owned, local_col, -1).astype(jnp.int32)
    return (weighted, row_total, target, columns, jnp.where(is_owned, slopes, 0.0))

def row_term(weighted, center_block, totals, columns, slopes):
    product = jnp.dot(weighted, center_block, preferred_element_type=jnp.float32)
    picked = jnp.take(center_block, jnp.clip(columns, 0, center_block.shape[0] - 1), axis=0).astype(jnp.float32)
    return product / totals[:, None] - (logit_scale * slopes)[:, None] * picked

def class_term(weighted, scaled, rows_hat, columns, slopes, class_count):
    product = lax.dot_general(weighted, scaled, (((0,), (0,)), ((), ())), preferred_element_type=jnp.float32)
    drop_index = jnp.where(columns >= 0, columns, class_count).astype(jnp.int32)
    updates = -(logit_scale * slopes)[:, None] * rows_hat.astype(jnp.float32)
    return product.at[drop_index].add(updates, mode='drop')

def reference(embeddings, labels, centers):
    inv_x, units_x, emb_hat = unit_rows(embeddings)
    inv_w, units_w, center_hat = unit_rows(centers)
    hat_blocks = center_hat.reshape(N_CLS, C_DEV, D)
    starts = jnp.arange(N_CLS, dtype=jnp.int32) * C_DEV
    zero_rows = jnp.zeros((BATCH,), jnp.float32)

    def forward(carry, block_item):
        center_block, class_base = block_item
        weighted, row_total, target, columns, slopes = score_block(emb_hat, labels, center_block, class_base)
        return ((carry[0] + row_total, carry[1] + target), None)
    (totals, targets), _ = lax.scan(forward, (zero_rows, zero_rows), (hat_blocks, starts))
    losses = jnp.log(totals) + logit_scale - targets
    scaled = (emb_hat.astype(jnp.float32) / totals[:, None]).astype(jnp.bfloat16)

    def backward(row_sums, block_item):
        center_block, class_base = block_item
        weighted, row_total, target, columns, slopes = score_block(emb_hat, labels, center_block, class_base)
        row_sums = row_sums + row_term(weighted, center_block, totals, columns, slopes)
        return (row_sums, class_term(weighted, scaled, emb_hat, columns, slopes, C_DEV))
    grad_hat_x, grad_blocks = lax.scan(backward, jnp.zeros((BATCH, D), jnp.float32), (hat_blocks, starts))
    grad_hat_w = grad_blocks.reshape(CLASSES, D)
    emb_grad = inv_x * (grad_hat_x - units_x * lax.optimization_barrier(jnp.sum(units_x * grad_hat_x, axis=1, keepdims=True)))
    center_grad = inv_w * (grad_hat_w - units_w * lax.optimization_barrier(jnp.sum(units_w * grad_hat_w, axis=1, keepdims=True)))
    return (losses, emb_grad, center_grad)
```

```python
import functools
import math

import jax
import jax.numpy as jnp
from jax import lax
from jax.experimental import pallas as pl
from jax.experimental.pallas import tpu as pltpu
from jax.sharding import PartitionSpec as P

MC = math.cos(0.5)
MS = math.sin(0.5)
EPS = 1e-06
NX, NY, NZ = 4, 2, 8
ROWS = 8
D = 512
C = 4096
B = 512
CB = 512
NCB = C // CB
F32 = jnp.float32
BF16 = jnp.bfloat16
ZOFF = (0, 1, 7, 2, 6, 3, 5, 4)


def pid(x, y, z):
    return x * (NY * NZ) + z * NY + y


def head_kernel(
    lab_ref, emb_ref, cen_ref,
    wt_ref, raw_ref, scaled_ref, coef_ref, lcol_ref, grad_ref, loss_ref,
    xg, lg, hat, hat_t, ehat, acc_n, acc_p, csend, crecv_y, crecv_x, crecv_z, ctot,
    dsend, drecv_x, drow, ysend, drecv_y, zown, zsend, drecv_z,
    cen_sem, send_sem, recv_sem,
):
    me = lax.axis_index("cls")
    x = me // (NY * NZ)
    z = (me % (NY * NZ)) // NY
    y = me % NY
    py = 1 - y
    ypeer = pid(x, py, z)
    xs = [(x + k) % NX for k in range(1, NX)]
    xpeers = [pid(v, y, z) for v in xs]
    zs = [(z + k) % NZ for k in ZOFF[1:]]
    zpeers = [pid(x, y, v) for v in zs]
    base = me * C

    def cen_copy(i):
        rows = pl.ds(i * CB, CB)
        return pltpu.make_async_copy(cen_ref.at[rows], raw_ref.at[rows], cen_sem.at[i])

    for i in range(NCB):
        cen_copy(i).start()

    barrier = pltpu.get_barrier_semaphore()
    for p in [ypeer] + xpeers + zpeers:
        pl.semaphore_signal(barrier, inc=1, device_id={"cls": p})

    lane = lax.broadcasted_iota(jnp.int32, (1, 128), 1)
    off = (y * NZ + z) * ROWS
    lrow = jnp.zeros((1, 128), jnp.int32)
    for r in range(ROWS):
        lrow = jnp.where(lane == off + r, lab_ref[r], lrow)
    lg[x, y, z] = lrow
    xg[x, y, z] = emb_ref[...]

    pl.semaphore_wait(barrier, 11)

    pending = []
    nsem = [0]

    def copy(src, dst, peer):
        i = nsem[0]
        nsem[0] += 1
        return pltpu.make_async_remote_copy(
            src_ref=src, dst_ref=dst, send_sem=send_sem.at[i], recv_sem=recv_sem.at[i],
            device_id={"cls": peer},
        )

    def go(src, dst, peer):
        c = copy(src, dst, peer)
        c.start()
        pending.append(c)
        return c

    ye = go(emb_ref, xg.at[x, y, z], ypeer)
    yl = go(lg.at[x, y, z], lg.at[x, y, z], ypeer)

    def norm_block(i):
        cen_copy(i).wait()
        rows = pl.ds(i * CB, CB)
        v = raw_ref[rows].astype(F32)
        inv = lax.rsqrt(jnp.sum(v * v, axis=1, keepdims=True) + EPS)
        hat[rows] = (v * inv).astype(BF16)

    def turn_block(i):
        rows = pl.ds(i * CB, CB)
        a = lax.broadcasted_iota(jnp.int32, (D, D), 0)
        b = lax.broadcasted_iota(jnp.int32, (D, D), 1)
        eye = jnp.where(a == b, 1.0, 0.0).astype(BF16)
        t = lax.dot_general(eye, hat[rows], (((1,), (1,)), ((), ())), preferred_element_type=F32)
        hat_t[i] = t.astype(BF16)

    norm_block(0)
    ye.wait_recv()
    yl.wait_recv()
    ze = [go(xg.at[x, :, z], xg.at[x, :, z], p) for p in zpeers]
    zl = [go(lg.at[x, :, z], lg.at[x, :, z], p) for p in zpeers]
    xe = []

    def forward(j):
        zj = (z + NZ - ZOFF[j]) % NZ
        for p in xpeers:
            xe.append(go(xg.at[x, :, zj], xg.at[x, :, zj], p))

    forward(0)
    for j in range(1, NZ):
        norm_block(j)
        ze[j - 1].wait_recv()
        forward(j)
    for c in zl:
        c.wait_recv()
    xl = [go(lg.at[x], lg.at[x], p) for p in xpeers]

    for i in range(NCB):
        turn_block(i)

    for c in xe + xl:
        c.wait_recv()

    labs = []
    for v in range(NX):
        e = xg[v].astype(F32)
        inv = lax.rsqrt(jnp.sum(e * e, axis=-1, keepdims=True) + EPS)
        ehat[pl.ds(v * 128, 128)] = (e * inv).reshape(128, D).astype(BF16)
        labs.append(jnp.sum(lg[v].reshape(NY * NZ, 128), axis=0, keepdims=True))
    lab = jnp.concatenate(labs, axis=1)
    lcol = lab - base
    owned = (lcol >= 0) & (lcol < C)
    lcol_ref[...] = jnp.broadcast_to(lcol, (8, B))

    def block(i, carry):
        t_acc, c_acc = carry
        rows = pl.ds(pl.multiple_of(i * CB, CB), CB)
        cos = lax.dot_general(
            hat[rows], ehat[...], (((1,), (1,)), ((), ())), preferred_element_type=F32
        )
        rid = lax.broadcasted_iota(jnp.int32, (CB, B), 0) + i * CB
        mask = rid == lcol
        c_acc += jnp.sum(jnp.where(mask, cos, 0.0).reshape(CB // 8, 8, B), axis=0)
        e = jnp.where(mask, 0.0, jnp.exp(64.0 * cos - 64.0))
        t_acc += jnp.sum(e.reshape(CB // 8, 8, B), axis=0)
        wt_ref[rows] = e.astype(BF16)
        return t_acc, c_acc

    zero = jnp.zeros((8, B), F32)
    t_acc, c_acc = lax.fori_loop(0, NCB, block, (zero, zero))
    t_part = jnp.sum(t_acc, axis=0, keepdims=True)
    tcos = jnp.sum(c_acc, axis=0, keepdims=True)
    tsin = jnp.sqrt(1.04 - tcos * tcos)
    shifted = tcos * MC - tsin * MS
    slope = jnp.where(owned, MC + MS * tcos / tsin, 0.0)
    et = jnp.where(owned, jnp.exp(64.0 * shifted - 64.0), 0.0)
    target = jnp.where(owned, 64.0 * shifted, 0.0)
    t_part = t_part + et
    for k in range(4):
        cols = slice(k * 128, (k + 1) * 128)
        csend[0, k : k + 1] = t_part[:, cols]
        csend[0, k + 4 : k + 5] = target[:, cols]
    cy = go(csend.at[0], crecv_y, ypeer)

    def n_block(i):
        rows = pl.ds(i * CB, CB)
        t = jnp.dot(hat_t[i], wt_ref[rows], preferred_element_type=F32)
        if i == 0:
            acc_n[...] = t
        else:
            acc_n[...] += t

    def p_block(i):
        rid = lax.broadcasted_iota(jnp.int32, (CB, B), 0) + i * CB
        hot = jnp.where(rid == lcol, 1.0, 0.0).astype(BF16)
        t = jnp.dot(hat_t[i], hot, preferred_element_type=F32)
        if i == 0:
            acc_p[...] = t
        else:
            acc_p[...] += t

    for i in range(4):
        n_block(i)
    cy.wait_recv()
    csend[1] = csend[0] + crecv_y[...]
    cx = [go(csend.at[1], crecv_x.at[k], p) for k, p in enumerate(xpeers)]
    for i in range(4, 8):
        n_block(i)
    p_block(0)
    for c in cx:
        c.wait_recv()
    csend[2] = csend[1] + crecv_x[0] + crecv_x[1] + crecv_x[2]
    cz = [go(csend.at[2], crecv_z.at[k], p) for k, p in enumerate(zpeers)]
    for i in range(1, 8):
        p_block(i)
    for c in cz:
        c.wait_recv()
    tot = csend[2]
    for k in range(7):
        tot = tot + crecv_z[k]
    ctot[...] = tot

    total = jnp.concatenate([ctot[k : k + 1] for k in range(4)], axis=1)
    inv_t = 1.0 / total
    coef_ref[...] = jnp.broadcast_to(slope * (et - total), (8, B))
    ca = 64.0 * inv_t
    cb = 64.0 * slope * (et * inv_t - 1.0)
    for k in range(4):
        cols = slice(k * 128, (k + 1) * 128)
        g = acc_n[:, cols] * ca[:, cols] + acc_p[:, cols] * cb[:, cols]
        acc_n[:, cols] = g
        dsend[k] = g.astype(BF16)
    dx = [go(dsend.at[v], drecv_x.at[k], p) for k, (v, p) in enumerate(zip(xs, xpeers))]

    for k in range(4):
        cols = slice(k * 128, (k + 1) * 128)
        col = jnp.broadcast_to(ca[:, cols], (128, 128)).T
        for j in range(4):
            dcols = slice(j * 128, (j + 1) * 128)
            v = ehat[pl.ds(k * 128, 128), dcols].astype(F32) * col
            scaled_ref[pl.ds(k * 128, 128), dcols] = v.astype(BF16)

    trow = ctot[pl.ds(x, 1)]
    grow = ctot[pl.ds(x + 4, 1)]
    lossv = jnp.log(trow) + 64.0 - grow
    lossv = jnp.broadcast_to(lossv, (8, 128))
    loss_ref[...] = pltpu.roll(lossv, (128 - off) % 128, 1)

    for c in dx:
        c.wait_recv()
    own = acc_n[:, pl.ds(pl.multiple_of(x * 128, 128), 128)]
    own = own + drecv_x[0].astype(F32) + drecv_x[1].astype(F32) + drecv_x[2].astype(F32)
    drow[...] = own.T.reshape(NY, 64, D)
    ysend[...] = drow[py].astype(BF16)
    dy = go(ysend, drecv_y, ypeer)
    dy.wait_recv()
    s = drow[y] + drecv_y[...].astype(F32)
    zown[...] = s.reshape(NZ, ROWS, D)
    zsend[...] = s.reshape(NZ, ROWS, D).astype(BF16)
    dz = [go(zsend.at[v], drecv_z.at[k], p) for k, (v, p) in enumerate(zip(zs, zpeers))]
    for c in dz:
        c.wait_recv()
    g = zown[z]
    for k in range(7):
        g = g + drecv_z[k].astype(F32)
    e = emb_ref[...].astype(F32)
    inv = lax.rsqrt(jnp.sum(e * e, axis=1, keepdims=True) + EPS)
    u = e * inv
    grad_ref[...] = inv * (g - u * jnp.sum(u * g, axis=1, keepdims=True))
    for c in pending:
        c.wait_send()


def class_kernel(
    lab_ref, wt_ref, raw_ref, scaled_ref, coef_ref, grad_ref, loss_ref,
    out_ref, gout_ref, lout_ref, buf, sem,
):
    gout_ref[...] = grad_ref[...]
    lout_ref[...] = loss_ref[...]
    copies = [None] * NCB
    for i in range(NCB):
        rows = slice(i * CB, (i + 1) * CB)
        w = wt_ref[rows]
        rid = lax.broadcasted_iota(jnp.int32, (CB, B), 0) + i * CB
        w = jnp.where(rid == lab_ref[0:1], coef_ref[0:1], w.astype(F32)).astype(BF16)
        g = jnp.dot(w, scaled_ref[...], preferred_element_type=F32)
        v = raw_ref[rows].astype(F32)
        inv = lax.rsqrt(jnp.sum(v * v, axis=1, keepdims=True) + EPS)
        dot = jnp.sum(v * g, axis=1, keepdims=True)
        if i >= 3:
            copies[i - 3].wait()
        buf[i % 3] = inv * g - (inv * inv * inv * dot) * v
        copies[i] = pltpu.make_async_copy(buf.at[i % 3], out_ref.at[rows], sem.at[i % 3])
        copies[i].start()
    for c in copies[-3:]:
        c.wait()


def per_device(embeddings, labels, centers):
    vm = pl.BlockSpec(memory_space=pltpu.VMEM)
    return pl.pallas_call(
        head_kernel,
        out_shape=(
            pltpu.VMEM((C, B), BF16),
            pltpu.VMEM((C, D), BF16),
            pltpu.VMEM((B, D), BF16),
            pltpu.VMEM((8, B), F32),
            pltpu.VMEM((8, B), jnp.int32),
            pltpu.VMEM((ROWS, D), F32),
            pltpu.VMEM((8, 128), F32),
        ),
        in_specs=[
            pl.BlockSpec(memory_space=pltpu.SMEM),
            vm,
            pl.BlockSpec(memory_space=pl.ANY),
        ],
        out_specs=(vm,) * 7,
        scratch_shapes=[
            pltpu.VMEM((NX, NY, NZ, ROWS, D), BF16),
            pltpu.VMEM((NX, NY, NZ, 1, 128), jnp.int32),
            pltpu.VMEM((C, D), BF16),
            pltpu.VMEM((NCB, D, CB), BF16),
            pltpu.VMEM((B, D), BF16),
            pltpu.VMEM((D, B), F32),
            pltpu.VMEM((D, B), F32),
            pltpu.VMEM((3, 8, 128), F32),
            pltpu.VMEM((8, 128), F32),
            pltpu.VMEM((3, 8, 128), F32),
            pltpu.VMEM((7, 8, 128), F32),
            pltpu.VMEM((8, 128), F32),
            pltpu.VMEM((NX, D, 128), BF16),
            pltpu.VMEM((3, D, 128), BF16),
            pltpu.VMEM((NY, 64, D), F32),
            pltpu.VMEM((64, D), BF16),
            pltpu.VMEM((64, D), BF16),
            pltpu.VMEM((NZ, ROWS, D), F32),
            pltpu.VMEM((NZ, ROWS, D), BF16),
            pltpu.VMEM((7, ROWS, D), BF16),
            pltpu.SemaphoreType.DMA((NCB,)),
            pltpu.SemaphoreType.DMA((70,)),
            pltpu.SemaphoreType.DMA((70,)),
        ],
        compiler_params=pltpu.CompilerParams(
            collective_id=0, has_side_effects=True, vmem_limit_bytes=40 * 1024 * 1024
        ),
        name="head",
    )(labels, embeddings, centers)


def whole(embeddings, labels, centers):
    wt, raw, scaled, coef, lcol, grad, loss = per_device(embeddings, labels, centers)
    vm = pl.BlockSpec(memory_space=pltpu.VMEM)
    out, grad, loss = pl.pallas_call(
        class_kernel,
        out_shape=(
            jax.ShapeDtypeStruct((C, D), F32),
            jax.ShapeDtypeStruct((ROWS, D), F32),
            jax.ShapeDtypeStruct((8, 128), F32),
        ),
        in_specs=[vm] * 7,
        out_specs=(pl.BlockSpec(memory_space=pl.ANY), vm, vm),
        scratch_shapes=[
            pltpu.VMEM((3, CB, D), F32),
            pltpu.SemaphoreType.DMA((3,)),
        ],
        compiler_params=pltpu.CompilerParams(vmem_limit_bytes=24 * 1024 * 1024),
        name="classes",
    )(lcol, wt, raw, scaled, coef, grad, loss)
    return loss[0, :ROWS], grad, out


def solution(mesh):
    in_specs = (P(("dp", "cls"), None), P(("dp", "cls")), P(("dp", "cls"), None))
    out_specs = (P(("dp", "cls")), P(("dp", "cls"), None), P(("dp", "cls"), None))
    return jax.shard_map(
        whole, mesh=mesh, in_specs=in_specs, out_specs=out_specs, check_vma=False
    )
```

```python
import functools
import math

import jax
import jax.numpy as jnp
from jax import lax
from jax.experimental import pallas as pl
from jax.experimental.pallas import tpu as pltpu
from jax.sharding import PartitionSpec as P

MC = math.cos(0.5)
MS = math.sin(0.5)
EPS = 1e-06
NX, NY, NZ = 4, 2, 8
ROWS = 8
D = 512
C = 4096
B = 512
CB = 512
NCB = C // CB
F32 = jnp.float32
BF16 = jnp.bfloat16
ZOFF = (0, 1, 7, 2, 6, 3, 5, 4)


def pid(x, y, z):
    return x * (NY * NZ) + z * NY + y


def head_kernel(
    lab_hbm, emb_hbm, cen_ref,
    out_ref, grad_ref, loss_ref,
    lab_ref, emb_ref, wt_ref, raw_ref, scaled_ref, coef_ref, xg, lg, hat, hat_t, ehat, acc_n, acc_p, csend, crecv_y, crecv_x, crecv_z, ctot,
    dsend, drecv_x, drow, ysend, drecv_y, zown, zsend, drecv_z,
    cen_sem, send_sem, recv_sem,
):
    me = lax.axis_index("cls")
    x = me // (NY * NZ)
    z = (me % (NY * NZ)) // NY
    y = me % NY
    py = 1 - y
    ypeer = pid(x, py, z)
    xs = [(x + k) % NX for k in range(1, NX)]
    xpeers = [pid(v, y, z) for v in xs]
    ypeers = [pid(x, py, (z + k) % NZ) for k in ZOFF]
    zs = [(z + k) % NZ for k in ZOFF[1:]]
    zpeers = [pid(x, y, v) for v in zs]
    base = me * C

    def cen_copy(i):
        rows = pl.ds(i * CB, CB)
        return pltpu.make_async_copy(cen_ref.at[rows], raw_ref.at[rows], cen_sem.at[i])

    small = [
        pltpu.make_async_copy(lab_hbm, lab_ref, cen_sem.at[NCB]),
        pltpu.make_async_copy(emb_hbm, emb_ref, cen_sem.at[NCB + 1]),
    ]
    for c in small:
        c.start()
    for i in range(NCB):
        cen_copy(i).start()

    barrier = pltpu.get_barrier_semaphore()
    for p in ypeers + xpeers + zpeers:
        pl.semaphore_signal(barrier, inc=1, device_id={"cls": p})

    lane = lax.broadcasted_iota(jnp.int32, (1, 128), 1)
    off = (y * NZ + z) * ROWS
    lrow = jnp.zeros((1, 128), jnp.int32)
    for c in small:
        c.wait()
    for r in range(ROWS):
        lrow = jnp.where(lane == off + r, lab_ref[r], lrow)
    lg[x, y, z] = lrow
    xg[x, y, z] = emb_ref[...]

    def norm_block(i):
        cen_copy(i).wait()
        rows = pl.ds(i * CB, CB)
        v = raw_ref[rows].astype(F32)
        inv = lax.rsqrt(jnp.sum(v * v, axis=1, keepdims=True) + EPS)
        hat[rows] = (v * inv).astype(BF16)

    def turn_block(i):
        rows = pl.ds(i * CB, CB)
        a = lax.broadcasted_iota(jnp.int32, (D, D), 0)
        b = lax.broadcasted_iota(jnp.int32, (D, D), 1)
        eye = jnp.where(a == b, 1.0, 0.0).astype(BF16)
        t = lax.dot_general(eye, hat[rows], (((1,), (1,)), ((), ())), preferred_element_type=F32)
        hat_t[i] = t.astype(BF16)

    for i in range(NCB):
        norm_block(i)
    pl.semaphore_wait(barrier, 18)

    pending = []
    nsem = [0]

    def copy(src, dst, peer):
        i = nsem[0]
        nsem[0] += 1
        return pltpu.make_async_remote_copy(
            src_ref=src, dst_ref=dst, send_sem=send_sem.at[i], recv_sem=recv_sem.at[i],
            device_id={"cls": peer},
        )

    def go(src, dst, peer):
        c = copy(src, dst, peer)
        c.start()
        pending.append(c)
        return c

    own_e, own_l = emb_ref, lg.at[x, y, z]
    arr = []
    for k, off_z in enumerate(ZOFF):
        yz = []
        if k:
            yz.append((y, zpeers[k - 1]))
        yz.append((py, ypeers[k]))
        for src_y, p in yz:
            ce = go(own_e, xg.at[x, y, z], p)
            cl = go(own_l, lg.at[x, y, z], p)
            arr.append((ce, cl, src_y, (z + NZ - off_z) % NZ))
    xe = []

    def forward(v, w):
        for p in xpeers:
            xe.append(go(xg.at[x, v, w], xg.at[x, v, w], p))

    forward(y, z)
    for j, (ce, cl, v, w) in enumerate(arr):
        if j % 2 == 0:
            turn_block(j // 2)
        ce.wait_recv()
        forward(v, w)
    for ce, cl, v, w in arr:
        cl.wait_recv()
    xl = [go(lg.at[x], lg.at[x], p) for p in xpeers]

    for c in xe + xl:
        c.wait_recv()

    labs = []
    for v in range(NX):
        e = xg[v].astype(F32)
        inv = lax.rsqrt(jnp.sum(e * e, axis=-1, keepdims=True) + EPS)
        ehat[pl.ds(v * 128, 128)] = (e * inv).reshape(128, D).astype(BF16)
        labs.append(jnp.sum(lg[v].reshape(NY * NZ, 128), axis=0, keepdims=True))
    lab = jnp.concatenate(labs, axis=1)
    lcol = lab - base
    owned = (lcol >= 0) & (lcol < C)

    def block(i, carry):
        t_acc, c_acc = carry
        rows = pl.ds(pl.multiple_of(i * CB, CB), CB)
        cos = lax.dot_general(
            hat[rows], ehat[...], (((1,), (1,)), ((), ())), preferred_element_type=F32
        )
        rid = lax.broadcasted_iota(jnp.int32, (CB, B), 0) + i * CB
        mask = rid == lcol
        c_acc += jnp.sum(jnp.where(mask, cos, 0.0).reshape(CB // 8, 8, B), axis=0)
        e = jnp.where(mask, 0.0, jnp.exp(64.0 * cos - 64.0))
        t_acc += jnp.sum(e.reshape(CB // 8, 8, B), axis=0)
        wt_ref[rows] = e.astype(BF16)
        return t_acc, c_acc

    zero = jnp.zeros((8, B), F32)
    t_acc, c_acc = lax.fori_loop(0, NCB, block, (zero, zero))
    t_part = jnp.sum(t_acc, axis=0, keepdims=True)
    tcos = jnp.sum(c_acc, axis=0, keepdims=True)
    tsin = jnp.sqrt(1.04 - tcos * tcos)
    shifted = tcos * MC - tsin * MS
    slope = jnp.where(owned, MC + MS * tcos / tsin, 0.0)
    et = jnp.where(owned, jnp.exp(64.0 * shifted - 64.0), 0.0)
    target = jnp.where(owned, 64.0 * shifted, 0.0)
    t_part = t_part + et
    for k in range(4):
        cols = slice(k * 128, (k + 1) * 128)
        csend[0, k : k + 1] = t_part[:, cols]
        csend[0, k + 4 : k + 5] = target[:, cols]
    cy = go(csend.at[0], crecv_y, ypeer)

    def n_block(i):
        rows = pl.ds(i * CB, CB)
        t = jnp.dot(hat_t[i], wt_ref[rows], preferred_element_type=F32)
        if i == 0:
            acc_n[...] = t
        else:
            acc_n[...] += t

    def p_block(i):
        rid = lax.broadcasted_iota(jnp.int32, (CB, B), 0) + i * CB
        hot = jnp.where(rid == lcol, 1.0, 0.0).astype(BF16)
        t = jnp.dot(hat_t[i], hot, preferred_element_type=F32)
        if i == 0:
            acc_p[...] = t
        else:
            acc_p[...] += t

    for i in range(4):
        n_block(i)
    cy.wait_recv()
    csend[1] = csend[0] + crecv_y[...]
    cx = [go(csend.at[1], crecv_x.at[k], p) for k, p in enumerate(xpeers)]
    for i in range(4, 8):
        n_block(i)
    p_block(0)
    for c in cx:
        c.wait_recv()
    csend[2] = csend[1] + crecv_x[0] + crecv_x[1] + crecv_x[2]
    cz = [go(csend.at[2], crecv_z.at[k], p) for k, p in enumerate(zpeers)]
    for i in range(1, 8):
        p_block(i)
    for c in cz:
        c.wait_recv()
    tot = csend[2]
    for k in range(7):
        tot = tot + crecv_z[k]
    ctot[...] = tot

    total = jnp.concatenate([ctot[k : k + 1] for k in range(4)], axis=1)
    inv_t = 1.0 / total
    coef_ref[...] = jnp.broadcast_to(slope * (et - total), (8, B))
    ca = 64.0 * inv_t
    cb = 64.0 * slope * (et * inv_t - 1.0)
    for k in range(4):
        cols = slice(k * 128, (k + 1) * 128)
        g = acc_n[:, cols] * ca[:, cols] + acc_p[:, cols] * cb[:, cols]
        acc_n[:, cols] = g
        dsend[k] = g.astype(BF16)
    dx = [go(dsend.at[v], drecv_x.at[k], p) for k, (v, p) in enumerate(zip(xs, xpeers))]

    for k in range(4):
        cols = slice(k * 128, (k + 1) * 128)
        col = jnp.broadcast_to(ca[:, cols], (128, 128)).T
        for j in range(4):
            dcols = slice(j * 128, (j + 1) * 128)
            v = ehat[pl.ds(k * 128, 128), dcols].astype(F32) * col
            scaled_ref[pl.ds(k * 128, 128), dcols] = v.astype(BF16)

    trow = ctot[pl.ds(x, 1)]
    grow = ctot[pl.ds(x + 4, 1)]
    lossv = jnp.log(trow) + 64.0 - grow
    lossv = jnp.broadcast_to(lossv, (8, 128))
    loss_ref[...] = pltpu.roll(lossv, (128 - off) % 128, 1)

    def class_block(i):
        rows = pl.ds(i * CB, CB)
        rid = lax.broadcasted_iota(jnp.int32, (CB, B), 0) + i * CB
        w = jnp.where(rid == lcol, coef_ref[0:1], wt_ref[rows].astype(F32)).astype(BF16)
        g = jnp.dot(w, scaled_ref[...], preferred_element_type=F32)
        v = raw_ref[rows].astype(F32)
        inv = lax.rsqrt(jnp.sum(v * v, axis=1, keepdims=True) + EPS)
        dot = jnp.sum(v * g, axis=1, keepdims=True)
        out_ref[rows] = inv * g - (inv * inv * inv * dot) * v

    for i in range(4):
        class_block(i)
    for c in dx:
        c.wait_recv()
    own = acc_n[:, pl.ds(pl.multiple_of(x * 128, 128), 128)]
    own = own + drecv_x[0].astype(F32) + drecv_x[1].astype(F32) + drecv_x[2].astype(F32)
    drow[...] = own.T.reshape(NY, 64, D)
    ysend[...] = drow[py].astype(BF16)
    dy = go(ysend, drecv_y, ypeer)
    for i in range(4, 6):
        class_block(i)
    dy.wait_recv()
    s = drow[y] + drecv_y[...].astype(F32)
    zown[...] = s.reshape(NZ, ROWS, D)
    zsend[...] = s.reshape(NZ, ROWS, D).astype(BF16)
    dz = [go(zsend.at[v], drecv_z.at[k], p) for k, (v, p) in enumerate(zip(zs, zpeers))]
    for i in range(6, 8):
        class_block(i)
    for c in dz:
        c.wait_recv()
    g = zown[z]
    for k in range(7):
        g = g + drecv_z[k].astype(F32)
    e = emb_ref[...].astype(F32)
    inv = lax.rsqrt(jnp.sum(e * e, axis=1, keepdims=True) + EPS)
    u = e * inv
    grad_ref[...] = inv * (g - u * jnp.sum(u * g, axis=1, keepdims=True))
    for c in pending:
        c.wait_send()


def write_kernel(val_ref, grad_ref, loss_ref, out_ref, gout_ref, lout_ref, sem):
    copies = []
    for i in range(NCB):
        rows = pl.ds(i * CB, CB)
        c = pltpu.make_async_copy(val_ref.at[rows], out_ref.at[rows], sem.at[i])
        c.start()
        copies.append(c)
    gout_ref[...] = grad_ref[...]
    lout_ref[...] = loss_ref[0:1, 0:ROWS]
    for c in copies:
        c.wait()


def whole(embeddings, labels, centers):
    vm = pl.BlockSpec(memory_space=pltpu.VMEM)
    hbm = pl.BlockSpec(memory_space=pltpu.HBM)
    val, grad, loss = pl.pallas_call(
        head_kernel,
        out_shape=(
            pltpu.VMEM((C, D), F32),
            pltpu.VMEM((ROWS, D), F32),
            pltpu.VMEM((8, 128), F32),
        ),
        in_specs=[hbm] * 3,
        out_specs=(vm,) * 3,
        scratch_shapes=[
            pltpu.SMEM((ROWS,), jnp.int32),
            pltpu.VMEM((ROWS, D), BF16),
            pltpu.VMEM((C, B), BF16),
            pltpu.VMEM((C, D), BF16),
            pltpu.VMEM((B, D), BF16),
            pltpu.VMEM((8, B), F32),
            pltpu.VMEM((NX, NY, NZ, ROWS, D), BF16),
            pltpu.VMEM((NX, NY, NZ, 1, 128), jnp.int32),
            pltpu.VMEM((C, D), BF16),
            pltpu.VMEM((NCB, D, CB), BF16),
            pltpu.VMEM((B, D), BF16),
            pltpu.VMEM((D, B), F32),
            pltpu.VMEM((D, B), F32),
            pltpu.VMEM((3, 8, 128), F32),
            pltpu.VMEM((8, 128), F32),
            pltpu.VMEM((3, 8, 128), F32),
            pltpu.VMEM((7, 8, 128), F32),
            pltpu.VMEM((8, 128), F32),
            pltpu.VMEM((NX, D, 128), BF16),
            pltpu.VMEM((3, D, 128), BF16),
            pltpu.VMEM((NY, 64, D), F32),
            pltpu.VMEM((64, D), BF16),
            pltpu.VMEM((64, D), BF16),
            pltpu.VMEM((NZ, ROWS, D), F32),
            pltpu.VMEM((NZ, ROWS, D), BF16),
            pltpu.VMEM((7, ROWS, D), BF16),
            pltpu.SemaphoreType.DMA((NCB + 2,)),
            pltpu.SemaphoreType.DMA((110,)),
            pltpu.SemaphoreType.DMA((110,)),
        ],
        compiler_params=pltpu.CompilerParams(
            collective_id=0, has_side_effects=True, vmem_limit_bytes=50 * 1024 * 1024
        ),
        name="head",
    )(labels, embeddings, centers)
    out, grad, loss = pl.pallas_call(
        write_kernel,
        out_shape=(
            jax.ShapeDtypeStruct((C, D), F32),
            jax.ShapeDtypeStruct((ROWS, D), F32),
            jax.ShapeDtypeStruct((1, ROWS), F32),
        ),
        in_specs=[vm] * 3,
        out_specs=(pl.BlockSpec(memory_space=pltpu.HBM), vm, vm),
        scratch_shapes=[pltpu.SemaphoreType.DMA((NCB,))],
        compiler_params=pltpu.CompilerParams(vmem_limit_bytes=4 * 1024 * 1024),
        name="write",
    )(val, grad, loss)
    return loss.reshape(ROWS), grad, out


def solution(mesh):
    in_specs = (P(("dp", "cls"), None), P(("dp", "cls")), P(("dp", "cls"), None))
    out_specs = (P(("dp", "cls")), P(("dp", "cls"), None), P(("dp", "cls"), None))
    return jax.shard_map(
        whole, mesh=mesh, in_specs=in_specs, out_specs=out_specs, check_vma=False
    )
```

```python
import functools
import math

import jax
import jax.numpy as jnp
from jax import lax
from jax.experimental import pallas as pl
from jax.experimental.pallas import tpu as pltpu
from jax.sharding import PartitionSpec as P

MC = math.cos(0.5)
MS = math.sin(0.5)
EPS = 1e-06
NX, NY, NZ = 4, 2, 8
ROWS = 8
D = 512
C = 4096
B = 512
CB = 512
NCB = C // CB
F32 = jnp.float32
BF16 = jnp.bfloat16
ZOFF = (0, 1, 7, 2, 6, 3, 5, 4)
KQ = (0, 1, 3, 2)
HB = B // 2
NK = 6
LOG2E = 64.0 / math.log(2.0)


def pid(x, y, z):
    return x * (NY * NZ) + z * NY + y


def class_rows(i, lcol_ref, coef_ref, wt_ref, raw_ref, scaled_ref):
    rows = slice(i * CB, (i + 1) * CB)
    rid = lax.broadcasted_iota(jnp.int32, (CB, B), 0) + i * CB
    w = jnp.where(rid == lcol_ref[0:1], coef_ref[0:1], wt_ref[rows].astype(F32)).astype(BF16)
    g = jnp.dot(w, scaled_ref[...], preferred_element_type=F32)
    v = raw_ref[rows].astype(F32)
    inv = lax.rsqrt(jnp.sum(v * v, axis=1, keepdims=True) + EPS)
    dot = jnp.sum(v * g, axis=1, keepdims=True)
    return inv * g - (inv * inv * inv * dot) * v


def head_kernel(
    lab_hbm, emb_hbm, cen_ref,
    out_ref, grad_ref, loss_ref, wt_ref, raw_ref, scaled_ref, coef_ref, lcol_ref,
    lab_ref, emb_ref, xg, lg, hat, hat_t, ehat, cosb,
    own_n, pt, csend, crecv_x, crecv_yz, ctot,
    psend, precv_x, prow, precv, dsend, drecv_x, drow, drow_b, drecv,
    cen_sem, send_sem, recv_sem,
):
    me = lax.axis_index("cls")
    x = me // (NY * NZ)
    z = (me % (NY * NZ)) // NY
    y = me % NY
    py = 1 - y
    planes = [(x + NX - k) % NX for k in KQ]
    xpeers = [pid(v, y, z) for v in planes[1:]]
    yz_ids = []
    for k in ZOFF:
        if k:
            yz_ids.append((y, k))
        yz_ids.append((py, k))
    yzpeers = [pid(x, v, (z + k) % NZ) for v, k in yz_ids]
    base = me * C

    def cen_copy(i):
        rows = pl.ds(i * CB, CB)
        return pltpu.make_async_copy(cen_ref.at[rows], raw_ref.at[rows], cen_sem.at[i])

    small = [
        pltpu.make_async_copy(lab_hbm, lab_ref, cen_sem.at[NCB]),
        pltpu.make_async_copy(emb_hbm, emb_ref, cen_sem.at[NCB + 1]),
    ]
    for c in small:
        c.start()
    for i in range(NCB):
        cen_copy(i).start()

    barrier = pltpu.get_barrier_semaphore()
    for p in yzpeers + xpeers:
        pl.semaphore_signal(barrier, inc=1, device_id={"cls": p})

    lane = lax.broadcasted_iota(jnp.int32, (1, 128), 1)
    off = (y * NZ + z) * ROWS
    lrow = jnp.zeros((1, 128), jnp.int32)
    for c in small:
        c.wait()
    for r in range(ROWS):
        lrow = jnp.where(lane == off + r, lab_ref[r], lrow)
    lg[y, z, x] = lrow
    xg[x, y, z] = emb_ref[...]

    def norm_block(i):
        cen_copy(i).wait()
        rows = pl.ds(i * CB, CB)
        v = raw_ref[rows].astype(F32)
        inv = lax.rsqrt(jnp.sum(v * v, axis=1, keepdims=True) + EPS)
        hat[rows] = (v * inv).astype(BF16)

    def turn_block(i):
        rows = pl.ds(i * CB, CB)
        a = lax.broadcasted_iota(jnp.int32, (D, D), 0)
        b = lax.broadcasted_iota(jnp.int32, (D, D), 1)
        eye = jnp.where(a == b, 1.0, 0.0).astype(BF16)
        t = lax.dot_general(eye, hat[rows], (((1,), (1,)), ((), ())), preferred_element_type=F32)
        hat_t[:, rows] = t.astype(BF16)

    for i in range(NCB):
        norm_block(i)
    pl.semaphore_wait(barrier, 18)

    pending = []
    nsem = [0]

    def go(src, dst, peer):
        i = nsem[0]
        nsem[0] += 1
        c = pltpu.make_async_remote_copy(
            src_ref=src, dst_ref=dst, send_sem=send_sem.at[i], recv_sem=recv_sem.at[i],
            device_id={"cls": peer},
        )
        c.start()
        pending.append(c)
        return c

    lsl = lg.at[y, z, x]
    xl = [go(lsl, lsl, p) for p in xpeers]
    ye = [go(emb_ref, xg.at[x, y, z], p) for p in yzpeers]
    xe = [[], [], []]

    def forward(v, w):
        for q, p in enumerate(xpeers):
            xe[q].append(go(xg.at[x, v, w], xg.at[x, v, w], p))

    forward(y, z)
    NL = 2
    for j, (c, (v, k)) in enumerate(zip(ye, yz_ids)):
        if j < NCB:
            turn_block(j)
        if j == NL:
            for cl in xl:
                cl.wait_recv()
            yl = [go(lg.at[y, z], lg.at[y, z], p) for p in yzpeers]
        c.wait_recv()
        forward(v, (z + NZ - k) % NZ)

    for c in yl:
        c.wait_recv()
    labs = [
        jnp.sum(lg[:, :, v].reshape(NY * NZ, 128), axis=0, keepdims=True) for v in planes
    ]
    lcol = jnp.concatenate(labs, axis=1) - base
    owned = (lcol >= 0) & (lcol < C)

    pacc = jnp.zeros((D, B), F32)
    for i in range(NCB):
        rid = lax.broadcasted_iota(jnp.int32, (CB, B), 0) + i * CB
        hot = jnp.where(rid == lcol, 1.0, 0.0).astype(BF16)
        pacc = pacc + jnp.dot(hat_t[:, i * CB : (i + 1) * CB], hot, preferred_element_type=F32)
    pt[...] = pacc.astype(BF16)
    for q in range(NX):
        psend[q] = pt[:, q * 128 : (q + 1) * 128]
    px = [go(psend.at[q + 1], precv_x.at[q], p) for q, p in enumerate(xpeers)]

    def emb_plane(q):
        e = xg[planes[q]].astype(F32)
        inv = lax.rsqrt(jnp.sum(e * e, axis=-1, keepdims=True) + EPS)
        ehat[q * 128 : (q + 1) * 128] = (e * inv).reshape(128, D).astype(BF16)

    def cos_chunk(h):
        cols = slice(h * HB, (h + 1) * HB)
        lc = lcol[:, cols]

        def score(i):
            cosb[i % 2] = lax.dot_general(
                hat[i * CB : (i + 1) * CB], ehat[cols],
                (((1,), (1,)), ((), ())), preferred_element_type=F32,
            )

        t_acc = jnp.zeros((8, HB), F32)
        score(0)
        for i in range(NCB):
            if i + 1 < NCB:
                score(i + 1)
            rid = lax.broadcasted_iota(jnp.int32, (CB, HB), 0)
            e = jnp.where(rid == lc - i * CB, 0.0, jnp.exp2(LOG2E * cosb[i % 2]))
            wt_ref[i * CB : (i + 1) * CB, cols] = e.astype(BF16)
            t_acc = t_acc + jnp.sum(e.reshape(CB // 8, 8, HB), axis=0)
        return t_acc

    def n_chunk(h):
        cols = slice(h * HB, (h + 1) * HB)
        t = jnp.dot(hat_t[...], wt_ref[:, cols], preferred_element_type=F32)
        if h == 0:
            own_n[...] = t[:, :128]
            dsend[1] = t[:, 128:].astype(BF16)
            return [go(dsend.at[1], drecv_x.at[0], xpeers[0])]
        dsend[2] = t[:, :128].astype(BF16)
        dsend[3] = t[:, 128:].astype(BF16)
        return [go(dsend.at[q], drecv_x.at[q - 1], xpeers[q - 1]) for q in (2, 3)]

    for c in xe[1]:
        c.wait_recv()
    emb_plane(0)
    emb_plane(1)
    t0 = cos_chunk(0)
    dx = n_chunk(0)
    for c in xe[0] + xe[2]:
        c.wait_recv()
    emb_plane(2)
    emb_plane(3)
    t1 = cos_chunk(1)
    t_part = jnp.sum(jnp.concatenate([t0, t1], axis=1), axis=0, keepdims=True)
    a = lax.broadcasted_iota(jnp.int32, (HB, HB), 0)
    b = lax.broadcasted_iota(jnp.int32, (HB, HB), 1)
    tc = []
    for h in range(2):
        cols = slice(h * HB, (h + 1) * HB)
        m = jnp.dot(ehat[cols], pt[:, cols], preferred_element_type=F32)
        tc.append(jnp.sum(jnp.where(a == b, m, 0.0), axis=0, keepdims=True))
    tcos = jnp.concatenate(tc, axis=1)
    tsin = jnp.sqrt(1.04 - tcos * tcos)
    shifted = tcos * MC - tsin * MS
    slope = jnp.where(owned, MC + MS * tcos / tsin, 0.0)
    et = jnp.where(owned, jnp.exp2(LOG2E * shifted), 0.0)
    t_part = t_part + et
    for q in range(NX):
        csend[0, pl.ds(planes[q], 1)] = t_part[:, q * 128 : (q + 1) * 128]
    cx = [go(csend.at[0], crecv_x.at[q], p) for q, p in enumerate(xpeers)]
    dx += n_chunk(1)
    for c in cx:
        c.wait_recv()
    csend[1] = csend[0] + crecv_x[0] + crecv_x[1] + crecv_x[2]
    cyz = [go(csend.at[1], crecv_yz.at[j], p) for j, p in enumerate(yzpeers)]
    for c in px:
        c.wait_recv()
    own = psend[0].astype(F32)
    for q in range(3):
        own = own + precv_x[q].astype(F32)
    prow[...] = own.T.reshape(NY, NZ, ROWS, D).astype(BF16)
    pyz = [
        go(prow.at[v, (z + k) % NZ], precv.at[j], p)
        for j, (p, (v, k)) in enumerate(zip(yzpeers, yz_ids))
    ]
    for c in dx:
        c.wait_recv()
    own = own_n[...]
    for q in range(3):
        own = own + drecv_x[q].astype(F32)
    rows = own.T.reshape(NY, NZ, ROWS, D)
    drow[...] = rows
    drow_b[...] = rows.astype(BF16)
    dyz = [
        go(drow_b.at[v, (z + k) % NZ], drecv.at[j], p)
        for j, (p, (v, k)) in enumerate(zip(yzpeers, yz_ids))
    ]
    for c in cyz:
        c.wait_recv()
    tot = csend[1]
    for j in range(15):
        tot = tot + crecv_yz[j]
    ctot[...] = tot

    total = jnp.concatenate([ctot[pl.ds(v, 1)] for v in planes], axis=1)
    ca = 64.0 / total
    coef = slope * (et - total)
    for k in range(4):
        cols = slice(k * 128, (k + 1) * 128)
        col = jnp.broadcast_to(ca[:, cols], (128, 128)).T
        for j in range(4):
            dcols = slice(j * 128, (j + 1) * 128)
            v = ehat[cols, dcols].astype(F32) * col
            scaled_ref[cols, dcols] = v.astype(BF16)

    coef_ref[...] = jnp.broadcast_to(coef, (8, B))
    lcol_ref[...] = jnp.broadcast_to(lcol, (8, B))
    for i in range(NK):
        out_ref[i * CB : (i + 1) * CB] = class_rows(
            i, lcol_ref, coef_ref, wt_ref, raw_ref, scaled_ref
        )
    for c in pyz:
        c.wait_recv()
    pick = prow[y, z].astype(F32)
    for j in range(15):
        pick = pick + precv[j].astype(F32)
    e = emb_ref[...].astype(F32)
    inv = lax.rsqrt(jnp.sum(e * e, axis=1, keepdims=True) + EPS)
    u = e * inv
    tc = jnp.sum(u.astype(BF16).astype(F32) * pick, axis=1, keepdims=True)
    ts = jnp.sqrt(1.04 - tc * tc)
    sh = tc * MC - ts * MS
    sl = MC + MS * tc / ts
    sub = lax.broadcasted_iota(jnp.int32, (ROWS, 128), 0)
    lan = lax.broadcasted_iota(jnp.int32, (ROWS, 128), 1)
    trow = jnp.broadcast_to(ctot[pl.ds(x, 1)], (ROWS, 128))
    tcol = jnp.sum(jnp.where(lan == sub + off, trow, 0.0), axis=1, keepdims=True)
    loss = jnp.log(tcol) - 64.0 * sh
    loss_ref[...] = jnp.sum(jnp.where(lan == sub, loss, 0.0), axis=0, keepdims=True)
    inv_t = 64.0 / tcol
    part = (sl * (jnp.exp2(LOG2E * sh) * inv_t - 64.0)) * pick
    for c in dyz:
        c.wait_recv()
    n = drow[y, z]
    for j in range(15):
        n = n + drecv[j].astype(F32)
    g = n * inv_t + part
    grad_ref[...] = inv * (g - u * jnp.sum(u * g, axis=1, keepdims=True))
    for c in pending:
        c.wait_send()


def write_kernel(
    val_ref, grad_ref, loss_ref, wt_ref, raw_ref, scaled_ref, coef_ref, lcol_ref,
    out_ref, gout_ref, lout_ref, buf, sem,
):
    copies = []

    def put(src, i):
        c = pltpu.make_async_copy(src, out_ref.at[pl.ds(i * CB, CB)], sem.at[i])
        c.start()
        copies.append(c)

    for i in range(NK):
        put(val_ref.at[pl.ds(i * CB, CB)], i)
    gout_ref[...] = grad_ref[...]
    lout_ref[...] = loss_ref[0:1, 0:ROWS]
    for i in range(NK, NCB):
        buf[i - NK] = class_rows(i, lcol_ref, coef_ref, wt_ref, raw_ref, scaled_ref)
        put(buf.at[i - NK], i)
    for c in copies:
        c.wait()


def whole(embeddings, labels, centers):
    vm = pl.BlockSpec(memory_space=pltpu.VMEM)
    hbm = pl.BlockSpec(memory_space=pltpu.HBM)
    made = pl.pallas_call(
        head_kernel,
        out_shape=(
            pltpu.VMEM((NK * CB, D), F32),
            pltpu.VMEM((ROWS, D), F32),
            pltpu.VMEM((1, 128), F32),
            pltpu.VMEM((C, B), BF16),
            pltpu.VMEM((C, D), BF16),
            pltpu.VMEM((B, D), BF16),
            pltpu.VMEM((8, B), F32),
            pltpu.VMEM((8, B), jnp.int32),
        ),
        in_specs=[hbm] * 3,
        out_specs=(vm,) * 8,
        scratch_shapes=[
            pltpu.SMEM((ROWS,), jnp.int32),
            pltpu.VMEM((ROWS, D), BF16),
            pltpu.VMEM((NX, NY, NZ, ROWS, D), BF16),
            pltpu.VMEM((NY, NZ, NX, 1, 128), jnp.int32),
            pltpu.VMEM((C, D), BF16),
            pltpu.VMEM((D, C), BF16),
            pltpu.VMEM((B, D), BF16),
            pltpu.VMEM((2, CB, HB), F32),
            pltpu.VMEM((D, 128), F32),
            pltpu.VMEM((D, B), BF16),
            pltpu.VMEM((2, NX, 128), F32),
            pltpu.VMEM((3, NX, 128), F32),
            pltpu.VMEM((15, NX, 128), F32),
            pltpu.VMEM((NX, 128), F32),
            pltpu.VMEM((NX, D, 128), BF16),
            pltpu.VMEM((3, D, 128), BF16),
            pltpu.VMEM((NY, NZ, ROWS, D), BF16),
            pltpu.VMEM((15, ROWS, D), BF16),
            pltpu.VMEM((NX, D, 128), BF16),
            pltpu.VMEM((3, D, 128), BF16),
            pltpu.VMEM((NY, NZ, ROWS, D), F32),
            pltpu.VMEM((NY, NZ, ROWS, D), BF16),
            pltpu.VMEM((15, ROWS, D), BF16),
            pltpu.SemaphoreType.DMA((NCB + 2,)),
            pltpu.SemaphoreType.DMA((140,)),
            pltpu.SemaphoreType.DMA((140,)),
        ],
        compiler_params=pltpu.CompilerParams(
            collective_id=0, has_side_effects=True, vmem_limit_bytes=48 * 1024 * 1024
        ),
        name="head",
    )(labels, embeddings, centers)
    out, grad, loss = pl.pallas_call(
        write_kernel,
        out_shape=(
            jax.ShapeDtypeStruct((C, D), F32),
            jax.ShapeDtypeStruct((ROWS, D), F32),
            jax.ShapeDtypeStruct((1, ROWS), F32),
        ),
        in_specs=[vm] * 8,
        out_specs=(pl.BlockSpec(memory_space=pltpu.HBM), vm, vm),
        scratch_shapes=[
            pltpu.VMEM((NCB - NK, CB, D), F32),
            pltpu.SemaphoreType.DMA((NCB,)),
        ],
        compiler_params=pltpu.CompilerParams(vmem_limit_bytes=12 * 1024 * 1024),
        name="write",
    )(*made)
    return loss.reshape(ROWS), grad, out


def solution(mesh):
    in_specs = (P(("dp", "cls"), None), P(("dp", "cls")), P(("dp", "cls"), None))
    out_specs = (P(("dp", "cls")), P(("dp", "cls"), None), P(("dp", "cls"), None))
    return jax.shard_map(
        whole, mesh=mesh, in_specs=in_specs, out_specs=out_specs, check_vma=False
    )
```

```python
import functools
import math

import jax
import jax.numpy as jnp
from jax import lax
from jax.experimental import pallas as pl
from jax.experimental.pallas import tpu as pltpu
from jax.sharding import PartitionSpec as P

MC = math.cos(0.5)
MS = math.sin(0.5)
EPS = 1e-06
NX, NY, NZ = 4, 2, 8
ROWS = 8
D = 512
C = 4096
B = 512
CB = 512
NCB = C // CB
F32 = jnp.float32
BF16 = jnp.bfloat16
ZOFF = (0, 1, 7, 2, 6, 3, 5, 4)
KQ = (0, 1, 3, 2)
HB = B // 2
NK = 6
LOG2E = 64.0 / math.log(2.0)


def pid(x, y, z):
    return x * (NY * NZ) + z * NY + y


def class_rows(i, lcol_ref, coef_ref, wt_ref, raw_ref, scaled_ref):
    rows = slice(i * CB, (i + 1) * CB)
    rid = lax.broadcasted_iota(jnp.int32, (CB, B), 0) + i * CB
    w = jnp.where(rid == lcol_ref[0:1], coef_ref[0:1], wt_ref[rows].astype(F32)).astype(BF16)
    g = jnp.dot(w, scaled_ref[...], preferred_element_type=F32)
    v = raw_ref[rows].astype(F32)
    inv = lax.rsqrt(jnp.sum(v * v, axis=1, keepdims=True) + EPS)
    dot = jnp.sum(v * g, axis=1, keepdims=True)
    return inv * g - (inv * inv * inv * dot) * v


def head_kernel(
    lab_hbm, emb_hbm, cen_ref,
    out_ref, grad_ref, loss_ref, wt_ref, raw_ref, scaled_ref, coef_ref, lcol_ref,
    lab_ref, emb_ref, xg, lg, hat, hat_t, ehat, cosb,
    own_n, pt, tacc, csend, crecv_x, crecv_yz, ctot,
    psend, precv_x, prow, precv, dsend, drecv_x, drow, drow_b, drecv,
    cen_sem, send_sem, recv_sem,
):
    me = lax.axis_index("cls")
    x = me // (NY * NZ)
    z = (me % (NY * NZ)) // NY
    y = me % NY
    py = 1 - y
    planes = [(x + NX - k) % NX for k in KQ]
    xpeers = [pid(v, y, z) for v in planes[1:]]
    yz_ids = []
    for k in ZOFF:
        if k:
            yz_ids.append((y, k))
        yz_ids.append((py, k))
    yzpeers = [pid(x, v, (z + k) % NZ) for v, k in yz_ids]
    base = me * C

    barrier = pltpu.get_barrier_semaphore()
    for p in yzpeers + xpeers:
        pl.semaphore_signal(barrier, inc=1, device_id={"cls": p})

    def cen_copy(i):
        rows = pl.ds(i * CB, CB)
        return pltpu.make_async_copy(cen_ref.at[rows], raw_ref.at[rows], cen_sem.at[i])

    small = [
        pltpu.make_async_copy(lab_hbm, lab_ref, cen_sem.at[NCB]),
        pltpu.make_async_copy(emb_hbm, emb_ref, cen_sem.at[NCB + 1]),
    ]
    for c in small:
        c.start()
    for i in range(NCB):
        cen_copy(i).start()

    lane = lax.broadcasted_iota(jnp.int32, (1, 128), 1)
    off = (y * NZ + z) * ROWS
    lrow = jnp.zeros((1, 128), jnp.int32)
    for c in small:
        c.wait()
    for r in range(ROWS):
        lrow = jnp.where(lane == off + r, lab_ref[r], lrow)
    lg[y, z, x] = lrow
    xg[x, y, z] = emb_ref[...]

    def norm_block(i):
        cen_copy(i).wait()
        rows = pl.ds(i * CB, CB)
        v = raw_ref[rows].astype(F32)
        inv = lax.rsqrt(jnp.sum(v * v, axis=1, keepdims=True) + EPS)
        hat[rows] = (v * inv).astype(BF16)

    def turn_block(i):
        rows = pl.ds(i * CB, CB)
        hat_t[:, rows] = hat[rows].T

    def apart(body):
        pl.when(me >= 0)(body)

    pl.semaphore_wait(barrier, 18)

    pending = []
    nsem = [0]

    def go(src, dst, peer):
        i = nsem[0]
        nsem[0] += 1
        c = pltpu.make_async_remote_copy(
            src_ref=src, dst_ref=dst, send_sem=send_sem.at[i], recv_sem=recv_sem.at[i],
            device_id={"cls": peer},
        )
        c.start()
        pending.append(c)
        return c

    lsl = lg.at[y, z, x]
    xl = [go(lsl, lsl, p) for p in xpeers]
    ye = [go(emb_ref, xg.at[x, y, z], p) for p in yzpeers]
    xe = [[], [], []]

    def forward(v, w):
        for q, p in enumerate(xpeers):
            xe[q].append(go(xg.at[x, v, w], xg.at[x, v, w], p))

    forward(y, z)
    for i in range(NCB):
        norm_block(i)
    NL = 4
    for j, (c, (v, k)) in enumerate(zip(ye, yz_ids)):
        if j < NCB:
            turn_block(j)
        if j == NL:
            for cl in xl:
                cl.wait_recv()
            yl = [go(lg.at[y, z], lg.at[y, z], p) for p in yzpeers]
        c.wait_recv()
        forward(v, (z + NZ - k) % NZ)

    for c in yl:
        c.wait_recv()
    labs = [
        jnp.sum(lg[:, :, v].reshape(NY * NZ, 128), axis=0, keepdims=True) for v in planes
    ]
    lcol = jnp.concatenate(labs, axis=1) - base
    owned = (lcol >= 0) & (lcol < C)

    def pick_labels():
        acc = jnp.zeros((D, B), F32)
        for i in range(NCB):
            rid = lax.broadcasted_iota(jnp.int32, (CB, B), 0) + i * CB
            hot = jnp.where(rid == lcol, 1.0, 0.0).astype(BF16)
            acc = acc + jnp.dot(
                hat_t[:, i * CB : (i + 1) * CB], hot, preferred_element_type=F32
            )
        p = acc.astype(BF16)
        pt[...] = p
        for q in range(NX):
            psend[q] = p[:, q * 128 : (q + 1) * 128]

    apart(pick_labels)
    px = [go(psend.at[q + 1], precv_x.at[q], p) for q, p in enumerate(xpeers)]

    def emb_plane(q):
        e = xg[planes[q]].astype(F32)
        inv = lax.rsqrt(jnp.sum(e * e, axis=-1, keepdims=True) + EPS)
        ehat[q * 128 : (q + 1) * 128] = (e * inv).reshape(128, D).astype(BF16)

    def cos_chunk(h):
        cols = slice(h * HB, (h + 1) * HB)
        lc = lcol[:, cols]

        def score(i):
            cosb[i % 2] = lax.dot_general(
                hat[i * CB : (i + 1) * CB], ehat[cols],
                (((1,), (1,)), ((), ())), preferred_element_type=F32,
            )

        t_acc = jnp.zeros((8, HB), F32)
        score(0)
        for i in range(NCB):
            if i + 1 < NCB:
                score(i + 1)
            rid = lax.broadcasted_iota(jnp.int32, (CB, HB), 0)
            e = jnp.where(rid == lc - i * CB, 0.0, jnp.exp2(LOG2E * cosb[i % 2]))
            wt_ref[i * CB : (i + 1) * CB, cols] = e.astype(BF16)
            t_acc = t_acc + jnp.sum(e.reshape(CB // 8, 8, HB), axis=0)
        tacc[:, cols] = t_acc

    def n_chunk(h):
        cols = slice(h * HB, (h + 1) * HB)
        t = jnp.dot(hat_t[...], wt_ref[:, cols], preferred_element_type=F32)
        if h == 0:
            own_n[...] = t[:, :128]
        else:
            dsend[2] = t[:, :128].astype(BF16)
        dsend[2 * h + 1] = t[:, 128:].astype(BF16)

    def n_send(q):
        return go(dsend.at[q], drecv_x.at[q - 1], xpeers[q - 1])

    for c in xe[1]:
        c.wait_recv()
    emb_plane(0)
    emb_plane(1)
    apart(lambda: cos_chunk(0))
    apart(lambda: n_chunk(0))
    dx = [n_send(1)]
    for c in xe[0] + xe[2]:
        c.wait_recv()
    emb_plane(2)
    emb_plane(3)
    apart(lambda: cos_chunk(1))
    t_part = jnp.sum(tacc[...], axis=0, keepdims=True)
    a = lax.broadcasted_iota(jnp.int32, (HB, HB), 0)
    b = lax.broadcasted_iota(jnp.int32, (HB, HB), 1)
    tc = []
    for h in range(2):
        cols = slice(h * HB, (h + 1) * HB)
        m = jnp.dot(ehat[cols], pt[:, cols], preferred_element_type=F32)
        tc.append(jnp.sum(jnp.where(a == b, m, 0.0), axis=0, keepdims=True))
    tcos = jnp.concatenate(tc, axis=1)
    tsin = jnp.sqrt(1.04 - tcos * tcos)
    shifted = tcos * MC - tsin * MS
    slope = jnp.where(owned, MC + MS * tcos / tsin, 0.0)
    et = jnp.where(owned, jnp.exp2(LOG2E * shifted), 0.0)
    t_part = t_part + et
    for q in range(NX):
        csend[0, pl.ds(planes[q], 1)] = t_part[:, q * 128 : (q + 1) * 128]
    cx = [go(csend.at[0], crecv_x.at[q], p) for q, p in enumerate(xpeers)]
    apart(lambda: n_chunk(1))
    dx += [n_send(2), n_send(3)]
    for c in cx:
        c.wait_recv()
    csend[1] = csend[0] + crecv_x[0] + crecv_x[1] + crecv_x[2]
    cyz = [go(csend.at[1], crecv_yz.at[j], p) for j, p in enumerate(yzpeers)]
    for c in px:
        c.wait_recv()
    own = psend[0].astype(F32)
    for q in range(3):
        own = own + precv_x[q].astype(F32)
    prow[...] = own.T.reshape(NY, NZ, ROWS, D).astype(BF16)
    pyz = [
        go(prow.at[v, (z + k) % NZ], precv.at[j], p)
        for j, (p, (v, k)) in enumerate(zip(yzpeers, yz_ids))
    ]
    for c in dx:
        c.wait_recv()
    own = own_n[...]
    for q in range(3):
        own = own + drecv_x[q].astype(F32)
    rows = own.T.reshape(NY, NZ, ROWS, D)
    drow[...] = rows
    drow_b[...] = rows.astype(BF16)
    dyz = [
        go(drow_b.at[v, (z + k) % NZ], drecv.at[j], p)
        for j, (p, (v, k)) in enumerate(zip(yzpeers, yz_ids))
    ]
    for c in cyz:
        c.wait_recv()
    tot = csend[1]
    for j in range(15):
        tot = tot + crecv_yz[j]
    ctot[...] = tot

    total = jnp.concatenate([ctot[pl.ds(v, 1)] for v in planes], axis=1)
    ca = 64.0 / total
    coef = slope * (et - total)
    for k in range(4):
        cols = slice(k * 128, (k + 1) * 128)
        col = jnp.broadcast_to(ca[:, cols], (128, 128)).T
        for j in range(4):
            dcols = slice(j * 128, (j + 1) * 128)
            v = ehat[cols, dcols].astype(F32) * col
            scaled_ref[cols, dcols] = v.astype(BF16)

    coef_ref[...] = jnp.broadcast_to(coef, (8, B))
    lcol_ref[...] = jnp.broadcast_to(lcol, (8, B))

    def class_block(i):
        out_ref[i * CB : (i + 1) * CB] = class_rows(
            i, lcol_ref, coef_ref, wt_ref, raw_ref, scaled_ref
        )

    for i in range(NK):
        apart(functools.partial(class_block, i))
    for c in pyz:
        c.wait_recv()
    pick = prow[y, z].astype(F32)
    for j in range(15):
        pick = pick + precv[j].astype(F32)
    e = emb_ref[...].astype(F32)
    inv = lax.rsqrt(jnp.sum(e * e, axis=1, keepdims=True) + EPS)
    u = e * inv
    tc = jnp.sum(u.astype(BF16).astype(F32) * pick, axis=1, keepdims=True)
    ts = jnp.sqrt(1.04 - tc * tc)
    sh = tc * MC - ts * MS
    sl = MC + MS * tc / ts
    sub = lax.broadcasted_iota(jnp.int32, (ROWS, 128), 0)
    lan = lax.broadcasted_iota(jnp.int32, (ROWS, 128), 1)
    trow = jnp.broadcast_to(ctot[pl.ds(x, 1)], (ROWS, 128))
    tcol = jnp.sum(jnp.where(lan == sub + off, trow, 0.0), axis=1, keepdims=True)
    loss = jnp.log(tcol) - 64.0 * sh
    loss_ref[...] = jnp.sum(jnp.where(lan == sub, loss, 0.0), axis=0, keepdims=True)
    inv_t = 64.0 / tcol
    part = (sl * (jnp.exp2(LOG2E * sh) * inv_t - 64.0)) * pick
    for c in dyz:
        c.wait_recv()
    n = drow[y, z]
    for j in range(15):
        n = n + drecv[j].astype(F32)
    g = n * inv_t + part
    grad_ref[...] = inv * (g - u * jnp.sum(u * g, axis=1, keepdims=True))
    for c in pending:
        c.wait_send()


def write_kernel(
    val_ref, grad_ref, loss_ref, wt_ref, raw_ref, scaled_ref, coef_ref, lcol_ref,
    out_ref, gout_ref, lout_ref, buf, sem,
):
    copies = []

    def put(src, i):
        c = pltpu.make_async_copy(src, out_ref.at[pl.ds(i * CB, CB)], sem.at[i])
        c.start()
        copies.append(c)

    for i in range(NK):
        put(val_ref.at[pl.ds(i * CB, CB)], i)
    gout_ref[...] = grad_ref[...]
    lout_ref[...] = loss_ref[0:1, 0:ROWS]
    for i in range(NK, NCB):
        buf[i - NK] = class_rows(i, lcol_ref, coef_ref, wt_ref, raw_ref, scaled_ref)
        put(buf.at[i - NK], i)
    for c in copies:
        c.wait()


def whole(embeddings, labels, centers):
    vm = pl.BlockSpec(memory_space=pltpu.VMEM)
    hbm = pl.BlockSpec(memory_space=pltpu.HBM)
    made = pl.pallas_call(
        head_kernel,
        out_shape=(
            pltpu.VMEM((NK * CB, D), F32),
            pltpu.VMEM((ROWS, D), F32),
            pltpu.VMEM((1, 128), F32),
            pltpu.VMEM((C, B), BF16),
            pltpu.VMEM((C, D), BF16),
            pltpu.VMEM((B, D), BF16),
            pltpu.VMEM((8, B), F32),
            pltpu.VMEM((8, B), jnp.int32),
        ),
        in_specs=[hbm] * 3,
        out_specs=(vm,) * 8,
        scratch_shapes=[
            pltpu.SMEM((ROWS,), jnp.int32),
            pltpu.VMEM((ROWS, D), BF16),
            pltpu.VMEM((NX, NY, NZ, ROWS, D), BF16),
            pltpu.VMEM((NY, NZ, NX, 1, 128), jnp.int32),
            pltpu.VMEM((C, D), BF16),
            pltpu.VMEM((D, C), BF16),
            pltpu.VMEM((B, D), BF16),
            pltpu.VMEM((2, CB, HB), F32),
            pltpu.VMEM((D, 128), F32),
            pltpu.VMEM((D, B), BF16),
            pltpu.VMEM((8, B), F32),
            pltpu.VMEM((2, NX, 128), F32),
            pltpu.VMEM((3, NX, 128), F32),
            pltpu.VMEM((15, NX, 128), F32),
            pltpu.VMEM((NX, 128), F32),
            pltpu.VMEM((NX, D, 128), BF16),
            pltpu.VMEM((3, D, 128), BF16),
            pltpu.VMEM((NY, NZ, ROWS, D), BF16),
            pltpu.VMEM((15, ROWS, D), BF16),
            pltpu.VMEM((NX, D, 128), BF16),
            pltpu.VMEM((3, D, 128), BF16),
            pltpu.VMEM((NY, NZ, ROWS, D), F32),
            pltpu.VMEM((NY, NZ, ROWS, D), BF16),
            pltpu.VMEM((15, ROWS, D), BF16),
            pltpu.SemaphoreType.DMA((NCB + 2,)),
            pltpu.SemaphoreType.DMA((140,)),
            pltpu.SemaphoreType.DMA((140,)),
        ],
        compiler_params=pltpu.CompilerParams(
            collective_id=0, has_side_effects=True, vmem_limit_bytes=48 * 1024 * 1024
        ),
        name="head",
    )(labels, embeddings, centers)
    out, grad, loss = pl.pallas_call(
        write_kernel,
        out_shape=(
            jax.ShapeDtypeStruct((C, D), F32),
            jax.ShapeDtypeStruct((ROWS, D), F32),
            jax.ShapeDtypeStruct((1, ROWS), F32),
        ),
        in_specs=[vm] * 8,
        out_specs=(pl.BlockSpec(memory_space=pltpu.HBM), vm, vm),
        scratch_shapes=[
            pltpu.VMEM((NCB - NK, CB, D), F32),
            pltpu.SemaphoreType.DMA((NCB,)),
        ],
        compiler_params=pltpu.CompilerParams(vmem_limit_bytes=12 * 1024 * 1024),
        name="write",
    )(*made)
    return loss.reshape(ROWS), grad, out


def solution(mesh):
    in_specs = (P(("dp", "cls"), None), P(("dp", "cls")), P(("dp", "cls"), None))
    out_specs = (P(("dp", "cls")), P(("dp", "cls"), None), P(("dp", "cls"), None))
    return jax.shard_map(
        whole, mesh=mesh, in_specs=in_specs, out_specs=out_specs, check_vma=False
    )
```

```python
import functools
import math

import jax
import jax.numpy as jnp
from jax import lax
from jax.experimental import pallas as pl
from jax.experimental.pallas import tpu as pltpu
from jax.sharding import PartitionSpec as P

MC = math.cos(0.5)
MS = math.sin(0.5)
EPS = 1e-06
NX, NY, NZ = 4, 2, 8
ROWS = 8
D = 512
C = 4096
B = 512
CB = 512
NCB = C // CB
F32 = jnp.float32
BF16 = jnp.bfloat16
ZOFF = (0, 1, 7, 2, 6, 3, 5, 4)
XY = ((1, 0), (3, 0), (2, 0), (0, 1), (1, 1), (3, 1), (2, 1))
HB = B // 2
NK = 7
LOG2E = 64.0 / math.log(2.0)


def pid(x, y, z):
    return x * (NY * NZ) + z * NY + y


def class_rows(i, lcol_ref, coef_ref, wt_ref, raw_ref, scaled_ref):
    rows = slice(i * CB, (i + 1) * CB)
    rid = lax.broadcasted_iota(jnp.int32, (CB, B), 0) + i * CB
    w = jnp.where(rid == lcol_ref[0:1], coef_ref[0:1], wt_ref[rows].astype(F32)).astype(BF16)
    g = jnp.dot(w, scaled_ref[...], preferred_element_type=F32)
    v = raw_ref[rows].astype(F32)
    inv = lax.rsqrt(jnp.sum(v * v, axis=1, keepdims=True) + EPS)
    dot = jnp.sum(v * g, axis=1, keepdims=True)
    return inv * g - (inv * inv * inv * dot) * v


def head_kernel(
    lab_hbm, emb_hbm, cen_ref,
    out_ref, grad_ref, loss_ref, wt_ref, raw_ref, scaled_ref, coef_ref, lcol_ref,
    lab_ref, emb_ref, xg, lg, hat, hat_t, ehat, cosb, lcolb, tacc,
    csend, crecv_xy, crecv_z, ctot,
    psend, precv_y, psum, precv_x, pz, precv_z,
    nsend, nown, nrecv, nz, nz_b, nrecv_z,
    cen_sem, send_sem, recv_sem,
):
    me = lax.axis_index("cls")
    x = me // (NY * NZ)
    z = (me % (NY * NZ)) // NY
    y = me % NY
    ys = (y, 1 - y)
    xk = {k: (x + k) % NX for k in range(NX)}
    zpeers = [pid(x, y, (z + k) % NZ) for k in ZOFF[1:]]
    ypeer = pid(x, ys[1], z)
    xypeers = [pid(xk[k], ys[h], z) for k, h in XY]
    base = me * C

    barrier = pltpu.get_barrier_semaphore()
    for p in zpeers + xypeers:
        pl.semaphore_signal(barrier, inc=1, device_id={"cls": p})

    def cen_copy(i):
        rows = pl.ds(i * CB, CB)
        return pltpu.make_async_copy(cen_ref.at[rows], raw_ref.at[rows], cen_sem.at[i])

    small = [
        pltpu.make_async_copy(lab_hbm, lab_ref, cen_sem.at[NCB]),
        pltpu.make_async_copy(emb_hbm, emb_ref, cen_sem.at[NCB + 1]),
    ]
    for c in small:
        c.start()
    for i in range(NCB):
        cen_copy(i).start()

    lane = lax.broadcasted_iota(jnp.int32, (1, 128), 1)
    off = (x % 2) * 64 + z * ROWS
    lrow = jnp.zeros((1, 128), jnp.int32)
    for c in small:
        c.wait()
    for r in range(ROWS):
        lrow = jnp.where(lane == off + r, lab_ref[r], lrow)
    lg[y, x, z] = lrow
    xg[y, x, z] = emb_ref[...]

    def norm_block(i):
        cen_copy(i).wait()
        rows = pl.ds(i * CB, CB)
        v = raw_ref[rows].astype(F32)
        inv = lax.rsqrt(jnp.sum(v * v, axis=1, keepdims=True) + EPS)
        hat[rows] = (v * inv).astype(BF16)

    def turn_block(i):
        rows = pl.ds(i * CB, CB)
        hat_t[:, rows] = hat[rows].T

    def apart(body):
        pl.when(me >= 0)(body)

    pl.semaphore_wait(barrier, 14)

    pending = []
    nsem = [0]

    def go(src, dst, peer):
        i = nsem[0]
        nsem[0] += 1
        c = pltpu.make_async_remote_copy(
            src_ref=src, dst_ref=dst, send_sem=send_sem.at[i], recv_sem=recv_sem.at[i],
            device_id={"cls": peer},
        )
        c.start()
        pending.append(c)
        return c

    lsl = lg.at[y, x, z]
    lz = [go(lsl, lsl, p) for p in zpeers]
    ez = [go(emb_ref, xg.at[y, x, z], p) for p in zpeers]
    xf = {}
    yf = {}
    xg2 = {}

    def zat(j):
        return (z + NZ - ZOFF[j]) % NZ

    def forward_x(j):
        blk = xg.at[y, x, zat(j)]
        for k in (1, 3, 2):
            xf[j, k] = go(blk, blk, pid(xk[k], y, z))

    def forward_y(k, j):
        blk = xg.at[y, (x + NX - k) % NX, zat(j)]
        yf[k, j] = go(blk, blk, ypeer)

    def on_y(j):
        yf[0, j].wait_recv()
        blk = xg.at[ys[1], x, zat(j)]
        for k in (1, 3):
            xg2[k, j] = go(blk, blk, pid(xk[k], y, z))

    forward_x(0)
    forward_y(0, 0)

    work = [functools.partial(norm_block, i) for i in range(NCB)]
    work += [functools.partial(turn_block, i) for i in range(NCB)]

    def do(n):
        for _ in range(min(n, len(work))):
            work.pop(0)()

    def on_z(j):
        ez[j - 1].wait_recv()
        forward_x(j)
        forward_y(0, j)

    def on_x(j):
        for k in (1, 3, 2):
            xf[j, k].wait_recv()
            if k == 2:
                forward_y(k, j)

    do(4)
    on_z(1)
    on_z(2)
    do(2)
    on_z(3)
    on_z(4)
    do(2)
    on_x(0)
    on_z(5)
    on_z(6)
    do(1)
    on_z(7)
    for c in lz:
        c.wait_recv()
    lxy = [go(lg.at[y, x], lg.at[y, x], p) for p in xypeers]
    for j in range(1, NZ):
        do(1)
        on_y(j - 1)
        on_x(j)
    do(NCB)
    on_y(NZ - 1)

    def lab_half(h):
        return [
            jnp.sum(lg[ys[h], 2 * p : 2 * p + 2].reshape(2 * NZ, 128), axis=0, keepdims=True)
            - base
            for p in range(2)
        ]

    for c in lxy[:3]:
        c.wait_recv()
    labs = lab_half(0)
    lcols = [jnp.concatenate(labs, axis=1)]

    for c in lxy[3:]:
        c.wait_recv()
    labs += lab_half(1)
    lcols.append(jnp.concatenate(labs[2:], axis=1))
    lcol = jnp.concatenate(labs, axis=1)
    owned = (lcol >= 0) & (lcol < C)
    for q in range(4):
        lcolb[q * 128 : (q + 1) * 128] = jnp.broadcast_to(labs[q].astype(F32), (128, 128)).T

    def send_py(k):
        return go(psend.at[1, xk[k]], precv_y.at[xk[k]], ypeer)

    px = []

    def take_py(k):
        py[k].wait_recv()
        v = psend[0, xk[k]].astype(F32) + precv_y[xk[k]].astype(F32)
        psum[xk[k]] = v.astype(BF16)
        if k:
            px.append(go(psum.at[xk[k]], precv_x.at[k - 1], pid(xk[k], y, z)))

    def pick_labels():
        acc = jnp.zeros((B, D), F32)
        lanef = lax.broadcasted_iota(jnp.int32, (1, 128), 1).astype(F32)
        for i in range(NCB):
            hot = jnp.concatenate(
                [
                    jnp.where(lcolb[...] == lanef + float(i * CB + g * 128), 1.0, 0.0)
                    for g in range(CB // 128)
                ],
                axis=1,
            ).astype(BF16)
            acc = acc + jnp.dot(
                hot, hat[i * CB : (i + 1) * CB], preferred_element_type=F32
            )
        psend[...] = acc.astype(BF16).reshape(2, NX, 64, D)

    apart(pick_labels)
    py = {k: send_py(k) for k in (2, 1, 3)}

    def emb_half(h):
        e = xg[ys[h]].astype(F32)
        inv = lax.rsqrt(jnp.sum(e * e, axis=-1, keepdims=True) + EPS)
        ehat[h * HB : (h + 1) * HB] = (e * inv).reshape(HB, D).astype(BF16)

    def cos_chunk(h):
        cols = slice(h * HB, (h + 1) * HB)
        lc = lcols[h]

        def score(i):
            cosb[i % 2] = lax.dot_general(
                hat[i * CB : (i + 1) * CB], ehat[cols],
                (((1,), (1,)), ((), ())), preferred_element_type=F32,
            )

        t_acc = jnp.zeros((8, HB), F32)
        score(0)
        for i in range(NCB):
            if i + 1 < NCB:
                score(i + 1)
            rid = lax.broadcasted_iota(jnp.int32, (CB, HB), 0)
            e = jnp.where(rid == lc - i * CB, 0.0, jnp.exp2(LOG2E * cosb[i % 2]))
            wt_ref[i * CB : (i + 1) * CB, cols] = e.astype(BF16)
            t_acc = t_acc + jnp.sum(e.reshape(CB // 8, 8, HB), axis=0)
        tacc[:, cols] = t_acc

    def n_chunk(h):
        cols = slice(h * HB, (h + 1) * HB)
        t = jnp.dot(hat_t[...], wt_ref[:, cols], preferred_element_type=F32)
        t = t.T.reshape(NX, 64, D)
        nsend[h] = t.astype(BF16)
        if h == 0:
            nown[...] = t

    def n_send(hh):
        return [
            go(nsend.at[h, xk[k]], nrecv.at[i], xypeers[i])
            for i, (k, h) in enumerate(XY)
            if h == hh
        ]

    emb_half(0)
    apart(lambda: cos_chunk(0))
    for j in range(NZ):
        yf[2, j].wait_recv()
        xg2[1, j].wait_recv()
        xg2[3, j].wait_recv()
    emb_half(1)
    apart(lambda: cos_chunk(1))
    t_part = jnp.sum(tacc[...], axis=0, keepdims=True)
    a = lax.broadcasted_iota(jnp.int32, (HB, HB), 0)
    b = lax.broadcasted_iota(jnp.int32, (HB, HB), 1)
    tc = []
    for h in range(2):
        m = lax.dot_general(
            ehat[h * HB : (h + 1) * HB], psend[h].reshape(HB, D),
            (((1,), (1,)), ((), ())), preferred_element_type=F32,
        )
        tc.append(jnp.sum(jnp.where(a == b, m, 0.0), axis=0, keepdims=True))
    tcos = jnp.concatenate(tc, axis=1)
    tsin = jnp.sqrt(1.04 - tcos * tcos)
    shifted = tcos * MC - tsin * MS
    slope = jnp.where(owned, MC + MS * tcos / tsin, 0.0)
    et = jnp.where(owned, jnp.exp2(LOG2E * shifted), 0.0)
    t_part = t_part + et
    where_t = [ys[0] * 2, ys[0] * 2 + 1, ys[1] * 2, ys[1] * 2 + 1]
    for q in range(4):
        csend[0, pl.ds(where_t[q], 1)] = t_part[:, q * 128 : (q + 1) * 128]
    cxy = [go(csend.at[0], crecv_xy.at[i], p) for i, p in enumerate(xypeers)]
    py[0] = send_py(0)
    take_py(2)
    apart(lambda: n_chunk(1))
    nx = n_send(1)
    take_py(1)
    apart(lambda: n_chunk(0))
    nx += n_send(0)
    take_py(3)
    for c in cxy:
        c.wait_recv()
    tot = csend[0]
    for i in range(7):
        tot = tot + crecv_xy[i]
    csend[1] = tot
    cz = [go(csend.at[1], crecv_z.at[i], p) for i, p in enumerate(zpeers)]
    take_py(0)
    for c in px:
        c.wait_recv()
    s = psum[x].astype(F32)
    for i in range(3):
        s = s + precv_x[i].astype(F32)
    pz[...] = s.astype(BF16).reshape(NZ, ROWS, D)
    pzc = [
        go(pz.at[(z + k) % NZ], precv_z.at[i], p)
        for i, (k, p) in enumerate(zip(ZOFF[1:], zpeers))
    ]
    for c in nx:
        c.wait_recv()
    s = nown[x]
    for i in range(7):
        s = s + nrecv[i].astype(F32)
    s = s.reshape(NZ, ROWS, D)
    nz[...] = s
    nz_b[...] = s.astype(BF16)
    nzc = [
        go(nz_b.at[(z + k) % NZ], nrecv_z.at[i], p)
        for i, (k, p) in enumerate(zip(ZOFF[1:], zpeers))
    ]
    for c in cz:
        c.wait_recv()
    tot = csend[1]
    for i in range(7):
        tot = tot + crecv_z[i]
    ctot[...] = tot

    total = jnp.concatenate([ctot[pl.ds(v, 1)] for v in where_t], axis=1)
    ca = 64.0 / total
    coef = slope * (et - total)
    for k in range(4):
        cols = slice(k * 128, (k + 1) * 128)
        col = jnp.broadcast_to(ca[:, cols], (128, 128)).T
        for j in range(4):
            dcols = slice(j * 128, (j + 1) * 128)
            v = ehat[cols, dcols].astype(F32) * col
            scaled_ref[cols, dcols] = v.astype(BF16)
    coef_ref[...] = jnp.broadcast_to(coef, (8, B))
    lcol_ref[...] = jnp.broadcast_to(lcol, (8, B))

    def class_block(i):
        out_ref[i * CB : (i + 1) * CB] = class_rows(
            i, lcol_ref, coef_ref, wt_ref, raw_ref, scaled_ref
        )

    for i in range(NK):
        apart(functools.partial(class_block, i))
    for c in pzc:
        c.wait_recv()
    pick = pz[z].astype(F32)
    for i in range(7):
        pick = pick + precv_z[i].astype(F32)
    e = emb_ref[...].astype(F32)
    inv = lax.rsqrt(jnp.sum(e * e, axis=1, keepdims=True) + EPS)
    u = e * inv
    tc = jnp.sum(u.astype(BF16).astype(F32) * pick, axis=1, keepdims=True)
    ts = jnp.sqrt(1.04 - tc * tc)
    sh = tc * MC - ts * MS
    sl = MC + MS * tc / ts
    sub = lax.broadcasted_iota(jnp.int32, (ROWS, 128), 0)
    lan = lax.broadcasted_iota(jnp.int32, (ROWS, 128), 1)
    trow = jnp.broadcast_to(ctot[pl.ds(y * 2 + x // 2, 1)], (ROWS, 128))
    tcol = jnp.sum(jnp.where(lan == sub + off, trow, 0.0), axis=1, keepdims=True)
    loss = jnp.log(tcol) - 64.0 * sh
    loss_ref[...] = jnp.sum(jnp.where(lan == sub, loss, 0.0), axis=0, keepdims=True)
    inv_t = 64.0 / tcol
    part = (sl * (jnp.exp2(LOG2E * sh) * inv_t - 64.0)) * pick
    for c in nzc:
        c.wait_recv()
    n = nz[z]
    for i in range(7):
        n = n + nrecv_z[i].astype(F32)
    g = n * inv_t + part
    grad_ref[...] = inv * (g - u * jnp.sum(u * g, axis=1, keepdims=True))
    for c in pending:
        c.wait_send()


def write_kernel(
    val_ref, grad_ref, loss_ref, wt_ref, raw_ref, scaled_ref, coef_ref, lcol_ref,
    out_ref, gout_ref, lout_ref, buf, lbuf, sem,
):
    copies = []

    def put(src, i):
        c = pltpu.make_async_copy(src, out_ref.at[pl.ds(i * CB, CB)], sem.at[i])
        c.start()
        copies.append(c)

    for i in range(NK):
        put(val_ref.at[pl.ds(i * CB, CB)], i)
    lbuf[...] = loss_ref[0:1, 0:ROWS]
    copies.append(pltpu.make_async_copy(grad_ref, gout_ref, sem.at[NCB]))
    copies.append(pltpu.make_async_copy(lbuf, lout_ref, sem.at[NCB + 1]))
    for c in copies[NK:]:
        c.start()
    for i in range(NK, NCB):
        buf[i - NK] = class_rows(i, lcol_ref, coef_ref, wt_ref, raw_ref, scaled_ref)
        put(buf.at[i - NK], i)
    for c in copies:
        c.wait()


def whole(embeddings, labels, centers):
    vm = pl.BlockSpec(memory_space=pltpu.VMEM)
    hbm = pl.BlockSpec(memory_space=pltpu.HBM)
    made = pl.pallas_call(
        head_kernel,
        out_shape=(
            pltpu.VMEM((NK * CB, D), F32),
            pltpu.VMEM((ROWS, D), F32),
            pltpu.VMEM((1, 128), F32),
            pltpu.VMEM((C, B), BF16),
            pltpu.VMEM((C, D), BF16),
            pltpu.VMEM((B, D), BF16),
            pltpu.VMEM((8, B), F32),
            pltpu.VMEM((8, B), jnp.int32),
        ),
        in_specs=[hbm] * 3,
        out_specs=(vm,) * 8,
        scratch_shapes=[
            pltpu.SMEM((ROWS,), jnp.int32),
            pltpu.VMEM((ROWS, D), BF16),
            pltpu.VMEM((NY, NX, NZ, ROWS, D), BF16),
            pltpu.VMEM((NY, NX, NZ, 1, 128), jnp.int32),
            pltpu.VMEM((C, D), BF16),
            pltpu.VMEM((D, C), BF16),
            pltpu.VMEM((B, D), BF16),
            pltpu.VMEM((2, CB, HB), F32),
            pltpu.VMEM((B, 128), F32),
            pltpu.VMEM((8, B), F32),
            pltpu.VMEM((2, 4, 128), F32),
            pltpu.VMEM((7, 4, 128), F32),
            pltpu.VMEM((7, 4, 128), F32),
            pltpu.VMEM((4, 128), F32),
            pltpu.VMEM((2, NX, 64, D), BF16),
            pltpu.VMEM((NX, 64, D), BF16),
            pltpu.VMEM((NX, 64, D), BF16),
            pltpu.VMEM((3, 64, D), BF16),
            pltpu.VMEM((NZ, ROWS, D), BF16),
            pltpu.VMEM((7, ROWS, D), BF16),
            pltpu.VMEM((2, NX, 64, D), BF16),
            pltpu.VMEM((NX, 64, D), F32),
            pltpu.VMEM((7, 64, D), BF16),
            pltpu.VMEM((NZ, ROWS, D), F32),
            pltpu.VMEM((NZ, ROWS, D), BF16),
            pltpu.VMEM((7, ROWS, D), BF16),
            pltpu.SemaphoreType.DMA((NCB + 2,)),
            pltpu.SemaphoreType.DMA((130,)),
            pltpu.SemaphoreType.DMA((130,)),
        ],
        compiler_params=pltpu.CompilerParams(
            collective_id=0, has_side_effects=True, vmem_limit_bytes=48 * 1024 * 1024
        ),
        name="head",
    )(labels, embeddings, centers)
    out, grad, loss = pl.pallas_call(
        write_kernel,
        out_shape=(
            jax.ShapeDtypeStruct((C, D), F32),
            jax.ShapeDtypeStruct((ROWS, D), F32),
            jax.ShapeDtypeStruct((1, ROWS), F32),
        ),
        in_specs=[vm] * 8,
        out_specs=(hbm,) * 3,
        scratch_shapes=[
            pltpu.VMEM((NCB - NK, CB, D), F32),
            pltpu.VMEM((1, ROWS), F32),
            pltpu.SemaphoreType.DMA((NCB + 2,)),
        ],
        compiler_params=pltpu.CompilerParams(vmem_limit_bytes=12 * 1024 * 1024),
        name="write",
    )(*made)
    return loss.reshape(ROWS), grad, out


def solution(mesh):
    in_specs = (P(("dp", "cls"), None), P(("dp", "cls")), P(("dp", "cls"), None))
    out_specs = (P(("dp", "cls")), P(("dp", "cls"), None), P(("dp", "cls"), None))
    return jax.shard_map(
        whole, mesh=mesh, in_specs=in_specs, out_specs=out_specs, check_vma=False
    )
```

```python
import functools
import math

import jax
import jax.numpy as jnp
from jax import lax
from jax.experimental import pallas as pl
from jax.experimental.pallas import tpu as pltpu
from jax.sharding import PartitionSpec as P

MC = math.cos(0.5)
MS = math.sin(0.5)
EPS = 1e-06
NX, NY, NZ = 4, 2, 8
ROWS = 8
D = 512
C = 4096
B = 512
CB = 512
NCB = C // CB
F32 = jnp.float32
BF16 = jnp.bfloat16
ZOFF = (0, 1, 7, 2, 6, 3, 5, 4)
XY = ((1, 0), (3, 0), (2, 0), (0, 1), (1, 1), (3, 1), (2, 1))
HB = B // 2
NK = 6
LOG2E = 64.0 / math.log(2.0)


def pid(x, y, z):
    return x * (NY * NZ) + z * NY + y


def class_rows(i, lcol_ref, coef_ref, wt_ref, raw_ref, scaled_ref):
    rows = slice(i * CB, (i + 1) * CB)
    rid = lax.broadcasted_iota(jnp.int32, (CB, B), 0) + i * CB
    w = jnp.where(rid == lcol_ref[0:1], coef_ref[0:1], wt_ref[rows].astype(F32)).astype(BF16)
    g = jnp.dot(w, scaled_ref[...], preferred_element_type=F32)
    v = raw_ref[rows].astype(F32)
    inv = lax.rsqrt(jnp.sum(v * v, axis=1, keepdims=True) + EPS)
    dot = jnp.sum(v * g, axis=1, keepdims=True)
    return inv * g - (inv * inv * inv * dot) * v


def head_kernel(
    lab_hbm, emb_hbm, cen_ref,
    out_ref, grad_ref, loss_ref, wt_ref, raw_ref, scaled_ref, coef_ref, lcol_ref,
    lab_ref, emb_ref, xg, lg, hat, hat_t, ehat, cosb, lcolb, tacc,
    csend, crecv_xy, crecv_z, ctot,
    psend, precv_y, precv_x13, psum, precv_x, pz, precv_z,
    nsend, nown, nrecv_a, nmid, nrecv, nz, nz_b, nrecv_z,
    cen_sem, send_sem, recv_sem,
):
    me = lax.axis_index("cls")
    x = me // (NY * NZ)
    z = (me % (NY * NZ)) // NY
    y = me % NY
    ys = (y, 1 - y)
    xk = {k: (x + k) % NX for k in range(NX)}
    zpeers = [pid(x, y, (z + k) % NZ) for k in ZOFF[1:]]
    ypeer = pid(x, ys[1], z)
    xypeers = [pid(xk[k], ys[h], z) for k, h in XY]
    base = me * C

    barrier = pltpu.get_barrier_semaphore()
    for p in zpeers + xypeers:
        pl.semaphore_signal(barrier, inc=1, device_id={"cls": p})

    def cen_copy(i):
        rows = pl.ds(i * CB, CB)
        return pltpu.make_async_copy(cen_ref.at[rows], raw_ref.at[rows], cen_sem.at[i])

    small = [
        pltpu.make_async_copy(lab_hbm, lab_ref, cen_sem.at[NCB]),
        pltpu.make_async_copy(emb_hbm, emb_ref, cen_sem.at[NCB + 1]),
    ]
    for c in small:
        c.start()
    for i in range(NCB):
        cen_copy(i).start()

    lane = lax.broadcasted_iota(jnp.int32, (1, 128), 1)
    off = (x % 2) * 64 + z * ROWS
    lrow = jnp.zeros((1, 128), jnp.int32)
    for c in small:
        c.wait()
    for r in range(ROWS):
        lrow = jnp.where(lane == off + r, lab_ref[r], lrow)
    lg[y, x, z] = lrow
    xg[y, x, z] = emb_ref[...]

    def norm_block(i):
        cen_copy(i).wait()
        rows = pl.ds(i * CB, CB)
        v = raw_ref[rows].astype(F32)
        inv = lax.rsqrt(jnp.sum(v * v, axis=1, keepdims=True) + EPS)
        hat[rows] = (v * inv).astype(BF16)

    def turn_block(i):
        rows = pl.ds(i * CB, CB)
        hat_t[:, rows] = hat[rows].T

    def apart(body):
        pl.when(me >= 0)(body)

    pl.semaphore_wait(barrier, 14)

    groups = []
    sent = []

    def group():
        groups.append(None)
        return len(groups) - 1

    def go(src, dst, peer, g):
        pltpu.make_async_remote_copy(
            src_ref=src, dst_ref=dst, send_sem=send_sem.at[0], recv_sem=recv_sem.at[g],
            device_id={"cls": peer},
        ).start()

    def arrive(g, ref):
        pltpu.make_async_copy(ref, ref, recv_sem.at[g]).wait()
        sent.append(ref)

    lsl = lg.at[y, x, z]
    lz = group()
    for p in zpeers:
        go(lsl, lsl, p, lz)
    ez = [group() for p in zpeers]
    for g, p in zip(ez, zpeers):
        go(emb_ref, xg.at[y, x, z], p, g)
    xf = [group() for j in range(NZ)]
    yf = [group() for j in range(NZ)]
    rest = group()

    def zat(j):
        return (z + NZ - ZOFF[j]) % NZ

    def forward_x(j):
        blk = xg.at[y, x, zat(j)]
        for k in (1, 3, 2):
            go(blk, blk, pid(xk[k], y, z), xf[j])

    def forward_y(k, j):
        blk = xg.at[y, (x + NX - k) % NX, zat(j)]
        go(blk, blk, ypeer, rest if k else yf[j])

    def on_y(j):
        arrive(yf[j], emb_ref)
        blk = xg.at[ys[1], x, zat(j)]
        for k in (1, 3):
            go(blk, blk, pid(xk[k], y, z), rest)

    forward_x(0)
    forward_y(0, 0)

    work = [functools.partial(norm_block, i) for i in range(NCB)]

    def do(n):
        for _ in range(min(n, len(work))):
            work.pop(0)()

    def on_z(j):
        arrive(ez[j - 1], emb_ref)
        forward_x(j)
        forward_y(0, j)

    def on_x(j):
        arrive(xf[j], xg.at[y, x, pl.ds(0, 3)])
        forward_y(2, j)

    do(NCB)
    on_z(1)
    on_z(2)
    on_z(3)
    on_z(4)
    on_x(0)
    on_z(5)
    on_z(6)
    on_z(7)
    arrive(lz, lg.at[y, x, pl.ds(0, 7)])
    lxy = [group(), group()]
    for i, p in enumerate(xypeers):
        go(lg.at[y, x], lg.at[y, x], p, lxy[min(i // 3, 1)])
    for j in range(1, NZ):
        on_x(j)
        on_y(j - 1)
    on_y(NZ - 1)

    def lab_half(h):
        return [
            jnp.sum(lg[ys[h], 2 * p : 2 * p + 2].reshape(2 * NZ, 128), axis=0, keepdims=True)
            - base
            for p in range(2)
        ]

    arrive(lxy[0], lg.at[y, pl.ds(0, 3)])
    labs = lab_half(0)
    lcols = [jnp.concatenate(labs, axis=1)]

    arrive(lxy[1], lg.at[y])
    labs += lab_half(1)
    lcols.append(jnp.concatenate(labs[2:], axis=1))
    lcol = jnp.concatenate(labs, axis=1)
    owned = (lcol >= 0) & (lcol < C)
    for q in range(4):
        lcolb[q * 128 : (q + 1) * 128] = jnp.broadcast_to(labs[q].astype(F32), (128, 128)).T

    py2, px13, px = group(), group(), group()

    def take_y2():
        arrive(py2, precv_y)
        v = psend[0, xk[2]].astype(F32) + precv_y[...].astype(F32)
        psum[0] = v.astype(BF16)
        go(psum.at[0], precv_x.at[0], pid(xk[2], y, z), px)

    def take_x13():
        arrive(px13, precv_x13)
        v = [
            psend[h, x].astype(F32) + precv_x13[0, h].astype(F32) + precv_x13[1, h].astype(F32)
            for h in range(2)
        ]
        psum[1] = v[1].astype(BF16)
        go(psum.at[1], precv_x.at[1], ypeer, px)
        psum[2] = v[0].astype(BF16)

    def pick_labels():
        acc = jnp.zeros((B, D), F32)
        lanef = lax.broadcasted_iota(jnp.int32, (1, 128), 1).astype(F32)
        for i in range(NCB):
            hot = jnp.concatenate(
                [
                    jnp.where(lcolb[...] == lanef + float(i * CB + g * 128), 1.0, 0.0)
                    for g in range(CB // 128)
                ],
                axis=1,
            ).astype(BF16)
            acc = acc + jnp.dot(
                hot, hat[i * CB : (i + 1) * CB], preferred_element_type=F32
            )
            turn_block(i)
        psend[...] = acc.astype(BF16).reshape(2, NX, 64, D)

    apart(pick_labels)
    go(psend.at[1, xk[2]], precv_y, ypeer, py2)
    for i, k in enumerate((1, 3)):
        go(psend.at[:, xk[k]], precv_x13.at[i], pid(xk[k], y, z), px13)

    def emb_half(h):
        e = xg[ys[h]].astype(F32)
        inv = lax.rsqrt(jnp.sum(e * e, axis=-1, keepdims=True) + EPS)
        ehat[h * HB : (h + 1) * HB] = (e * inv).reshape(HB, D).astype(BF16)

    def cos_chunk(h):
        cols = slice(h * HB, (h + 1) * HB)
        lc = lcols[h]

        def score(i):
            cosb[i % 2] = lax.dot_general(
                hat[i * CB : (i + 1) * CB], ehat[cols],
                (((1,), (1,)), ((), ())), preferred_element_type=F32,
            )

        t_acc = jnp.zeros((8, HB), F32)
        score(0)
        for i in range(NCB):
            if i + 1 < NCB:
                score(i + 1)
            rid = lax.broadcasted_iota(jnp.int32, (CB, HB), 0)
            e = jnp.where(rid == lc - i * CB, 0.0, jnp.exp2(LOG2E * cosb[i % 2]))
            wt_ref[i * CB : (i + 1) * CB, cols] = e.astype(BF16)
            t_acc = t_acc + jnp.sum(e.reshape(CB // 8, 8, HB), axis=0)
        tacc[:, cols] = t_acc

    def n_chunk(h):
        cols = slice(h * HB, (h + 1) * HB)
        t = jnp.dot(hat_t[...], wt_ref[:, cols], preferred_element_type=F32)
        t = t.T.reshape(NX, 64, D)
        nsend[h] = t.astype(BF16)
        if h == 0:
            nown[...] = t

    emb_half(0)
    apart(lambda: cos_chunk(0))
    arrive(rest, xg.at[ys[1], pl.ds(0, 3)])
    emb_half(1)
    apart(lambda: cos_chunk(1))
    t_part = jnp.sum(tacc[...], axis=0, keepdims=True)
    a = lax.broadcasted_iota(jnp.int32, (HB, HB), 0)
    b = lax.broadcasted_iota(jnp.int32, (HB, HB), 1)
    tc = []
    for h in range(2):
        m = lax.dot_general(
            ehat[h * HB : (h + 1) * HB], psend[h].reshape(HB, D),
            (((1,), (1,)), ((), ())), preferred_element_type=F32,
        )
        tc.append(jnp.sum(jnp.where(a == b, m, 0.0), axis=0, keepdims=True))
    tcos = jnp.concatenate(tc, axis=1)
    tsin = jnp.sqrt(1.04 - tcos * tcos)
    shifted = tcos * MC - tsin * MS
    slope = jnp.where(owned, MC + MS * tcos / tsin, 0.0)
    et = jnp.where(owned, jnp.exp2(LOG2E * shifted), 0.0)
    t_part = t_part + et
    where_t = [ys[0] * 2, ys[0] * 2 + 1, ys[1] * 2, ys[1] * 2 + 1]
    for q in range(4):
        csend[0, pl.ds(where_t[q], 1)] = t_part[:, q * 128 : (q + 1) * 128]
    cxy = group()
    for i, p in enumerate(xypeers):
        go(csend.at[0], crecv_xy.at[i], p, cxy)
    take_y2()
    apart(lambda: n_chunk(1))
    take_x13()
    na, nx = group(), group()
    for i, k in enumerate((1, 3)):
        go(nsend.at[1, xk[k]], nrecv_a.at[i], pid(xk[k], y, z), na)
    go(nsend.at[1, xk[2]], nrecv.at[0], pid(xk[2], ys[1], z), nx)
    apart(lambda: n_chunk(0))
    for k in (1, 3, 2):
        go(nsend.at[0, xk[k]], nrecv.at[k], pid(xk[k], y, z), nx)
    arrive(cxy, crecv_xy)
    tot = csend[0]
    for i in range(7):
        tot = tot + crecv_xy[i]
    csend[1] = tot
    cz = group()
    for i, p in enumerate(zpeers):
        go(csend.at[1], crecv_z.at[i], p, cz)
    arrive(na, nrecv_a)
    v = nsend[1, x].astype(F32) + nrecv_a[0].astype(F32) + nrecv_a[1].astype(F32)
    nmid[...] = v.astype(BF16)
    go(nmid, nrecv.at[4], ypeer, nx)
    arrive(px, precv_x)
    s = psum[2].astype(F32) + precv_x[0].astype(F32) + precv_x[1].astype(F32)
    pz[...] = s.astype(BF16).reshape(NZ, ROWS, D)
    pzc = group()
    for i, (k, p) in enumerate(zip(ZOFF[1:], zpeers)):
        go(pz.at[(z + k) % NZ], precv_z.at[i], p, pzc)
    arrive(nx, nrecv)
    s = nown[x]
    for i in range(5):
        s = s + nrecv[i].astype(F32)
    s = s.reshape(NZ, ROWS, D)
    nz[...] = s
    nz_b[...] = s.astype(BF16)
    nzc = group()
    for i, (k, p) in enumerate(zip(ZOFF[1:], zpeers)):
        go(nz_b.at[(z + k) % NZ], nrecv_z.at[i], p, nzc)
    arrive(cz, crecv_z)
    tot = csend[1]
    for i in range(7):
        tot = tot + crecv_z[i]
    ctot[...] = tot

    total = jnp.concatenate([ctot[pl.ds(v, 1)] for v in where_t], axis=1)
    ca = 64.0 / total
    coef = slope * (et - total)
    for k in range(4):
        cols = slice(k * 128, (k + 1) * 128)
        col = jnp.broadcast_to(ca[:, cols], (128, 128)).T
        for j in range(4):
            dcols = slice(j * 128, (j + 1) * 128)
            v = ehat[cols, dcols].astype(F32) * col
            scaled_ref[cols, dcols] = v.astype(BF16)
    coef_ref[...] = jnp.broadcast_to(coef, (8, B))
    lcol_ref[...] = jnp.broadcast_to(lcol, (8, B))

    def class_block(i):
        out_ref[i * CB : (i + 1) * CB] = class_rows(
            i, lcol_ref, coef_ref, wt_ref, raw_ref, scaled_ref
        )

    for i in range(NK):
        apart(functools.partial(class_block, i))
    arrive(pzc, precv_z)
    pick = pz[z].astype(F32)
    for i in range(7):
        pick = pick + precv_z[i].astype(F32)
    e = emb_ref[...].astype(F32)
    inv = lax.rsqrt(jnp.sum(e * e, axis=1, keepdims=True) + EPS)
    u = e * inv
    tc = jnp.sum(u.astype(BF16).astype(F32) * pick, axis=1, keepdims=True)
    ts = jnp.sqrt(1.04 - tc * tc)
    sh = tc * MC - ts * MS
    sl = MC + MS * tc / ts
    sub = lax.broadcasted_iota(jnp.int32, (ROWS, 128), 0)
    lan = lax.broadcasted_iota(jnp.int32, (ROWS, 128), 1)
    trow = jnp.broadcast_to(ctot[pl.ds(y * 2 + x // 2, 1)], (ROWS, 128))
    tcol = jnp.sum(jnp.where(lan == sub + off, trow, 0.0), axis=1, keepdims=True)
    loss = jnp.log(tcol) - 64.0 * sh
    loss_ref[...] = jnp.sum(jnp.where(lan == sub, loss, 0.0), axis=0, keepdims=True)
    inv_t = 64.0 / tcol
    part = (sl * (jnp.exp2(LOG2E * sh) * inv_t - 64.0)) * pick
    arrive(nzc, nrecv_z)
    n = nz[z]
    for i in range(7):
        n = n + nrecv_z[i].astype(F32)
    g = n * inv_t + part
    grad_ref[...] = inv * (g - u * jnp.sum(u * g, axis=1, keepdims=True))
    for ref in sent:
        pltpu.make_async_copy(ref, ref, send_sem.at[0]).wait()


def write_kernel(
    val_ref, grad_ref, loss_ref, wt_ref, raw_ref, scaled_ref, coef_ref, lcol_ref,
    out_ref, gout_ref, lout_ref, buf, lbuf, sem,
):
    copies = []

    def put(src, i):
        c = pltpu.make_async_copy(src, out_ref.at[pl.ds(i * CB, CB)], sem.at[i])
        c.start()
        copies.append(c)

    for i in range(NK):
        put(val_ref.at[pl.ds(i * CB, CB)], i)
    lbuf[...] = loss_ref[0:1, 0:ROWS]
    copies.append(pltpu.make_async_copy(grad_ref, gout_ref, sem.at[NCB]))
    copies.append(pltpu.make_async_copy(lbuf, lout_ref, sem.at[NCB + 1]))
    for c in copies[NK:]:
        c.start()
    for i in range(NK, NCB):
        buf[i - NK] = class_rows(i, lcol_ref, coef_ref, wt_ref, raw_ref, scaled_ref)
        put(buf.at[i - NK], i)
    for c in copies:
        c.wait()


def whole(embeddings, labels, centers):
    vm = pl.BlockSpec(memory_space=pltpu.VMEM)
    hbm = pl.BlockSpec(memory_space=pltpu.HBM)
    made = pl.pallas_call(
        head_kernel,
        out_shape=(
            pltpu.VMEM((NK * CB, D), F32),
            pltpu.VMEM((ROWS, D), F32),
            pltpu.VMEM((1, 128), F32),
            pltpu.VMEM((C, B), BF16),
            pltpu.VMEM((C, D), BF16),
            pltpu.VMEM((B, D), BF16),
            pltpu.VMEM((8, B), F32),
            pltpu.VMEM((8, B), jnp.int32),
        ),
        in_specs=[hbm] * 3,
        out_specs=(vm,) * 8,
        scratch_shapes=[
            pltpu.SMEM((ROWS,), jnp.int32),
            pltpu.VMEM((ROWS, D), BF16),
            pltpu.VMEM((NY, NX, NZ, ROWS, D), BF16),
            pltpu.VMEM((NY, NX, NZ, 1, 128), jnp.int32),
            pltpu.VMEM((C, D), BF16),
            pltpu.VMEM((D, C), BF16),
            pltpu.VMEM((B, D), BF16),
            pltpu.VMEM((2, CB, HB), F32),
            pltpu.VMEM((B, 128), F32),
            pltpu.VMEM((8, B), F32),
            pltpu.VMEM((2, 4, 128), F32),
            pltpu.VMEM((7, 4, 128), F32),
            pltpu.VMEM((7, 4, 128), F32),
            pltpu.VMEM((4, 128), F32),
            pltpu.VMEM((2, NX, 64, D), BF16),
            pltpu.VMEM((64, D), BF16),
            pltpu.VMEM((2, 2, 64, D), BF16),
            pltpu.VMEM((3, 64, D), BF16),
            pltpu.VMEM((2, 64, D), BF16),
            pltpu.VMEM((NZ, ROWS, D), BF16),
            pltpu.VMEM((7, ROWS, D), BF16),
            pltpu.VMEM((2, NX, 64, D), BF16),
            pltpu.VMEM((NX, 64, D), F32),
            pltpu.VMEM((2, 64, D), BF16),
            pltpu.VMEM((64, D), BF16),
            pltpu.VMEM((5, 64, D), BF16),
            pltpu.VMEM((NZ, ROWS, D), F32),
            pltpu.VMEM((NZ, ROWS, D), BF16),
            pltpu.VMEM((7, ROWS, D), BF16),
            pltpu.SemaphoreType.DMA((NCB + 2,)),
            pltpu.SemaphoreType.DMA((1,)),
            pltpu.SemaphoreType.DMA((38,)),
        ],
        compiler_params=pltpu.CompilerParams(
            collective_id=0, has_side_effects=True, vmem_limit_bytes=48 * 1024 * 1024
        ),
        name="head",
    )(labels, embeddings, centers)
    out, grad, loss = pl.pallas_call(
        write_kernel,
        out_shape=(
            jax.ShapeDtypeStruct((C, D), F32),
            jax.ShapeDtypeStruct((ROWS, D), F32),
            jax.ShapeDtypeStruct((1, ROWS), F32),
        ),
        in_specs=[vm] * 8,
        out_specs=(hbm,) * 3,
        scratch_shapes=[
            pltpu.VMEM((NCB - NK, CB, D), F32),
            pltpu.VMEM((1, ROWS), F32),
            pltpu.SemaphoreType.DMA((NCB + 2,)),
        ],
        compiler_params=pltpu.CompilerParams(vmem_limit_bytes=12 * 1024 * 1024),
        name="write",
    )(*made)
    return loss.reshape(ROWS), grad, out


def solution(mesh):
    in_specs = (P(("dp", "cls"), None), P(("dp", "cls")), P(("dp", "cls"), None))
    out_specs = (P(("dp", "cls")), P(("dp", "cls"), None), P(("dp", "cls"), None))
    return jax.shard_map(
        whole, mesh=mesh, in_specs=in_specs, out_specs=out_specs, check_vma=False
    )
```

```python
import functools
import math

import jax
import jax.numpy as jnp
from jax import lax
from jax.experimental import pallas as pl
from jax.experimental.pallas import tpu as pltpu
from jax.sharding import PartitionSpec as P

MC = math.cos(0.5)
MS = math.sin(0.5)
EPS = 1e-06
NX, NY, NZ = 4, 2, 8
ROWS = 8
D = 512
C = 4096
B = 512
CB = 512
NCB = C // CB
F32 = jnp.float32
BF16 = jnp.bfloat16
ZOFF = (0, 1, 7, 2, 6, 3, 5, 4)
XY = ((1, 0), (3, 0), (2, 0), (0, 1), (1, 1), (3, 1), (2, 1))
HB = B // 2
NK = 5
HALVES = (slice(0, D // 2), slice(D // 2, D))
LOG2E = 64.0 / math.log(2.0)


def pid(x, y, z):
    return x * (NY * NZ) + z * NY + y


def class_rows(i, lcol_ref, coef_ref, wt_ref, raw_ref, scaled_ref):
    rows = slice(i * CB, (i + 1) * CB)
    rid = lax.broadcasted_iota(jnp.int32, (CB, B), 0) + i * CB
    w = jnp.where(rid == lcol_ref[0:1], coef_ref[0:1], wt_ref[rows].astype(F32)).astype(BF16)
    g = jnp.dot(w, scaled_ref[...], preferred_element_type=F32)
    v = raw_ref[rows].astype(F32)
    inv = lax.rsqrt(jnp.sum(v * v, axis=1, keepdims=True) + EPS)
    dot = jnp.sum(v * g, axis=1, keepdims=True)
    return inv * g - (inv * inv * inv * dot) * v


def head_kernel(
    lab_hbm, emb_hbm, cen_ref,
    out_ref, grad_ref, loss_ref, wt_ref, raw_ref, scaled_ref, coef_ref, lcol_ref,
    lab_ref, emb_ref, xg, lg, hat, hat_t, ehat, cosb, lcolb, tacc,
    csend, crecv_xy, crecv_z, ctot,
    psend, precv_y, precv_x13, psum, precv_x, pz, precv_z,
    nsend, nown, nrecv_a, nmid, nrecv, nz, nz_b, nrecv_z,
    cen_sem, send_sem, recv_sem,
):
    me = lax.axis_index("cls")
    x = me // (NY * NZ)
    z = (me % (NY * NZ)) // NY
    y = me % NY
    ys = (y, 1 - y)
    xk = {k: (x + k) % NX for k in range(NX)}
    zpeers = [pid(x, y, (z + k) % NZ) for k in ZOFF[1:]]
    ypeer = pid(x, ys[1], z)
    xypeers = [pid(xk[k], ys[h], z) for k, h in XY]
    base = me * C

    barrier = pltpu.get_barrier_semaphore()
    for p in zpeers + xypeers:
        pl.semaphore_signal(barrier, inc=1, device_id={"cls": p})

    def cen_copy(i):
        rows = pl.ds(i * CB, CB)
        return pltpu.make_async_copy(cen_ref.at[rows], raw_ref.at[rows], cen_sem.at[i])

    small = [
        pltpu.make_async_copy(lab_hbm, lab_ref, cen_sem.at[NCB]),
        pltpu.make_async_copy(emb_hbm, emb_ref, cen_sem.at[NCB + 1]),
    ]
    for c in small:
        c.start()
    for i in range(NCB):
        cen_copy(i).start()

    lane = lax.broadcasted_iota(jnp.int32, (1, 128), 1)
    off = (x % 2) * 64 + z * ROWS
    lrow = jnp.zeros((1, 128), jnp.int32)
    for c in small:
        c.wait()
    for r in range(ROWS):
        lrow = jnp.where(lane == off + r, lab_ref[r], lrow)
    lg[y, x, z] = lrow
    xg[y, x, z] = emb_ref[...]

    def norm_block(i):
        cen_copy(i).wait()
        rows = pl.ds(i * CB, CB)
        v = raw_ref[rows].astype(F32)
        inv = lax.rsqrt(jnp.sum(v * v, axis=1, keepdims=True) + EPS)
        hat[rows] = (v * inv).astype(BF16)

    def turn_block(i):
        rows = pl.ds(i * CB, CB)
        hat_t[:, rows] = hat[rows].T

    def apart(body):
        pl.when(me >= 0)(body)

    pl.semaphore_wait(barrier, 14)

    groups = []
    sent = []

    def group():
        groups.append(None)
        return len(groups) - 1

    def go(src, dst, peer, g):
        pltpu.make_async_remote_copy(
            src_ref=src, dst_ref=dst, send_sem=send_sem.at[0], recv_sem=recv_sem.at[g],
            device_id={"cls": peer},
        ).start()

    def arrive(g, ref):
        pltpu.make_async_copy(ref, ref, recv_sem.at[g]).wait()
        sent.append(ref)

    lsl = lg.at[y, x, z]
    lz = group()
    for p in zpeers:
        go(lsl, lsl, p, lz)
    ez = [group() for p in zpeers]
    for g, p in zip(ez, zpeers):
        go(emb_ref, xg.at[y, x, z], p, g)
    xf = [group() for j in range(NZ)]
    yf = [group() for j in range(NZ)]
    rest = group()

    def zat(j):
        return (z + NZ - ZOFF[j]) % NZ

    def forward_x(j):
        blk = xg.at[y, x, zat(j)]
        for k in (1, 3, 2):
            go(blk, blk, pid(xk[k], y, z), xf[j])

    def forward_y(k, j):
        blk = xg.at[y, (x + NX - k) % NX, zat(j)]
        go(blk, blk, ypeer, rest if k else yf[j])

    def on_y(j):
        arrive(yf[j], emb_ref)
        blk = xg.at[ys[1], x, zat(j)]
        for k in (1, 3):
            go(blk, blk, pid(xk[k], y, z), rest)

    forward_x(0)
    forward_y(0, 0)

    work = [functools.partial(norm_block, i) for i in range(NCB)]

    def do(n):
        for _ in range(min(n, len(work))):
            work.pop(0)()

    def on_z(j):
        arrive(ez[j - 1], emb_ref)
        forward_x(j)
        forward_y(0, j)

    def on_x(j):
        arrive(xf[j], xg.at[y, x, pl.ds(0, 3)])
        forward_y(2, j)

    do(NCB)
    on_z(1)
    on_z(2)
    on_z(3)
    on_z(4)
    on_x(0)
    on_z(5)
    on_z(6)
    on_z(7)
    arrive(lz, lg.at[y, x, pl.ds(0, 7)])
    lxy = [group(), group()]
    for i, p in enumerate(xypeers):
        go(lg.at[y, x], lg.at[y, x], p, lxy[min(i // 3, 1)])
    for j in range(1, NZ):
        on_x(j)
        on_y(j - 1)
    on_y(NZ - 1)

    def lab_half(h):
        return [
            jnp.sum(lg[ys[h], 2 * p : 2 * p + 2].reshape(2 * NZ, 128), axis=0, keepdims=True)
            - base
            for p in range(2)
        ]

    arrive(lxy[0], lg.at[y, pl.ds(0, 3)])
    labs = lab_half(0)
    lcols = [jnp.concatenate(labs, axis=1)]

    arrive(lxy[1], lg.at[y])
    labs += lab_half(1)
    lcols.append(jnp.concatenate(labs[2:], axis=1))
    lcol = jnp.concatenate(labs, axis=1)
    owned = (lcol >= 0) & (lcol < C)
    for q in range(4):
        lcolb[q * 128 : (q + 1) * 128] = jnp.broadcast_to(labs[q].astype(F32), (128, 128)).T

    py2, px13, px = group(), group(), group()

    def take_y2():
        arrive(py2, precv_y)
        v = psend[0, xk[2]].astype(F32) + precv_y[...].astype(F32)
        psum[0] = v.astype(BF16)
        go(psum.at[0], precv_x.at[0], pid(xk[2], y, z), px)

    def take_x13():
        arrive(px13, precv_x13)
        v = [
            psend[h, x].astype(F32) + precv_x13[0, h].astype(F32) + precv_x13[1, h].astype(F32)
            for h in range(2)
        ]
        psum[1] = v[1].astype(BF16)
        go(psum.at[1], precv_x.at[1], ypeer, px)
        psum[2] = v[0].astype(BF16)

    def pick_labels():
        acc = jnp.zeros((B, D), F32)
        lanef = lax.broadcasted_iota(jnp.int32, (1, 128), 1).astype(F32)
        for i in range(NCB):
            hot = jnp.concatenate(
                [
                    jnp.where(lcolb[...] == lanef + float(i * CB + g * 128), 1.0, 0.0)
                    for g in range(CB // 128)
                ],
                axis=1,
            ).astype(BF16)
            acc = acc + jnp.dot(
                hot, hat[i * CB : (i + 1) * CB], preferred_element_type=F32
            )
            turn_block(i)
        psend[...] = acc.astype(BF16).reshape(2, NX, 64, D)

    apart(pick_labels)
    go(psend.at[1, xk[2]], precv_y, ypeer, py2)
    for i, k in enumerate((1, 3)):
        go(psend.at[:, xk[k]], precv_x13.at[i], pid(xk[k], y, z), px13)

    def emb_half(h):
        e = xg[ys[h]].astype(F32)
        inv = lax.rsqrt(jnp.sum(e * e, axis=-1, keepdims=True) + EPS)
        ehat[h * HB : (h + 1) * HB] = (e * inv).reshape(HB, D).astype(BF16)

    def cos_chunk(h):
        cols = slice(h * HB, (h + 1) * HB)
        lc = lcols[h]

        def score(i):
            cosb[i % 2] = lax.dot_general(
                hat[i * CB : (i + 1) * CB], ehat[cols],
                (((1,), (1,)), ((), ())), preferred_element_type=F32,
            )

        t_acc = jnp.zeros((8, HB), F32)
        score(0)
        for i in range(NCB):
            if i + 1 < NCB:
                score(i + 1)
            rid = lax.broadcasted_iota(jnp.int32, (CB, HB), 0)
            e = jnp.where(rid == lc - i * CB, 0.0, jnp.exp2(LOG2E * cosb[i % 2]))
            wt_ref[i * CB : (i + 1) * CB, cols] = e.astype(BF16)
            t_acc = t_acc + jnp.sum(e.reshape(CB // 8, 8, HB), axis=0)
        tacc[:, cols] = t_acc

    def n_chunk(h):
        cols = slice(h * HB, (h + 1) * HB)
        t = jnp.dot(hat_t[...], wt_ref[:, cols], preferred_element_type=F32)
        t = t.T.reshape(NX, 64, D)
        nsend[h] = t.astype(BF16)
        if h == 0:
            nown[...] = t

    emb_half(0)
    apart(lambda: cos_chunk(0))
    arrive(rest, xg.at[ys[1], pl.ds(0, 3)])
    emb_half(1)
    apart(lambda: cos_chunk(1))
    t_part = jnp.sum(tacc[...], axis=0, keepdims=True)
    a = lax.broadcasted_iota(jnp.int32, (HB, HB), 0)
    b = lax.broadcasted_iota(jnp.int32, (HB, HB), 1)
    tc = []
    for h in range(2):
        m = lax.dot_general(
            ehat[h * HB : (h + 1) * HB], psend[h].reshape(HB, D),
            (((1,), (1,)), ((), ())), preferred_element_type=F32,
        )
        tc.append(jnp.sum(jnp.where(a == b, m, 0.0), axis=0, keepdims=True))
    tcos = jnp.concatenate(tc, axis=1)
    tsin = jnp.sqrt(1.04 - tcos * tcos)
    shifted = tcos * MC - tsin * MS
    slope = jnp.where(owned, MC + MS * tcos / tsin, 0.0)
    et = jnp.where(owned, jnp.exp2(LOG2E * shifted), 0.0)
    t_part = t_part + et
    where_t = [ys[0] * 2, ys[0] * 2 + 1, ys[1] * 2, ys[1] * 2 + 1]
    for q in range(4):
        csend[0, pl.ds(where_t[q], 1)] = t_part[:, q * 128 : (q + 1) * 128]
    cxy = group()
    for i, p in enumerate(xypeers):
        go(csend.at[0], crecv_xy.at[i], p, cxy)
    take_y2()
    apart(lambda: n_chunk(1))
    na, nx = (group(), group()), group()
    for h, lanes in enumerate(HALVES):
        for i, k in enumerate((1, 3)):
            src = nsend.at[1, xk[k], :, lanes]
            go(src, nrecv_a.at[i, :, lanes], pid(xk[k], y, z), na[h])
    go(nsend.at[1, xk[2]], nrecv.at[0], pid(xk[2], ys[1], z), nx)
    take_x13()
    apart(lambda: n_chunk(0))
    for k in (1, 3, 2):
        go(nsend.at[0, xk[k]], nrecv.at[k], pid(xk[k], y, z), nx)
    arrive(cxy, crecv_xy)
    tot = csend[0]
    for i in range(7):
        tot = tot + crecv_xy[i]
    csend[1] = tot
    cz = group()
    for i, p in enumerate(zpeers):
        go(csend.at[1], crecv_z.at[i], p, cz)
    for h, lanes in enumerate(HALVES):
        arrive(na[h], nrecv_a.at[:, :, lanes])
        v = nsend[1, x, :, lanes].astype(F32)
        v = v + nrecv_a[0, :, lanes].astype(F32) + nrecv_a[1, :, lanes].astype(F32)
        nmid[:, lanes] = v.astype(BF16)
        go(nmid.at[:, lanes], nrecv.at[4, :, lanes], ypeer, nx)
    arrive(px, precv_x)
    s = psum[2].astype(F32) + precv_x[0].astype(F32) + precv_x[1].astype(F32)
    pz[...] = s.astype(BF16).reshape(NZ, ROWS, D)
    pzc = group()
    for i, (k, p) in enumerate(zip(ZOFF[1:], zpeers)):
        go(pz.at[(z + k) % NZ], precv_z.at[i], p, pzc)
    arrive(nx, nrecv)
    s = nown[x]
    for i in range(5):
        s = s + nrecv[i].astype(F32)
    s = s.reshape(NZ, ROWS, D)
    nz[...] = s
    nz_b[...] = s.astype(BF16)
    nzc = group()
    for i, (k, p) in enumerate(zip(ZOFF[1:], zpeers)):
        go(nz_b.at[(z + k) % NZ], nrecv_z.at[i], p, nzc)
    arrive(cz, crecv_z)
    tot = csend[1]
    for i in range(7):
        tot = tot + crecv_z[i]
    ctot[...] = tot

    total = jnp.concatenate([ctot[pl.ds(v, 1)] for v in where_t], axis=1)
    ca = 64.0 / total
    coef = slope * (et - total)
    for k in range(4):
        cols = slice(k * 128, (k + 1) * 128)
        col = jnp.broadcast_to(ca[:, cols], (128, 128)).T
        for j in range(4):
            dcols = slice(j * 128, (j + 1) * 128)
            v = ehat[cols, dcols].astype(F32) * col
            scaled_ref[cols, dcols] = v.astype(BF16)
    coef_ref[...] = jnp.broadcast_to(coef, (8, B))
    lcol_ref[...] = jnp.broadcast_to(lcol, (8, B))

    def class_block(i):
        out_ref[i * CB : (i + 1) * CB] = class_rows(
            i, lcol_ref, coef_ref, wt_ref, raw_ref, scaled_ref
        )

    for i in range(NK):
        apart(functools.partial(class_block, i))
    arrive(pzc, precv_z)
    pick = pz[z].astype(F32)
    for i in range(7):
        pick = pick + precv_z[i].astype(F32)
    e = emb_ref[...].astype(F32)
    inv = lax.rsqrt(jnp.sum(e * e, axis=1, keepdims=True) + EPS)
    u = e * inv
    tc = jnp.sum(u.astype(BF16).astype(F32) * pick, axis=1, keepdims=True)
    ts = jnp.sqrt(1.04 - tc * tc)
    sh = tc * MC - ts * MS
    sl = MC + MS * tc / ts
    sub = lax.broadcasted_iota(jnp.int32, (ROWS, 128), 0)
    lan = lax.broadcasted_iota(jnp.int32, (ROWS, 128), 1)
    trow = jnp.broadcast_to(ctot[pl.ds(y * 2 + x // 2, 1)], (ROWS, 128))
    tcol = jnp.sum(jnp.where(lan == sub + off, trow, 0.0), axis=1, keepdims=True)
    loss = jnp.log(tcol) - 64.0 * sh
    loss_ref[...] = jnp.sum(jnp.where(lan == sub, loss, 0.0), axis=0, keepdims=True)
    inv_t = 64.0 / tcol
    part = (sl * (jnp.exp2(LOG2E * sh) * inv_t - 64.0)) * pick
    arrive(nzc, nrecv_z)
    n = nz[z]
    for i in range(7):
        n = n + nrecv_z[i].astype(F32)
    g = n * inv_t + part
    grad_ref[...] = inv * (g - u * jnp.sum(u * g, axis=1, keepdims=True))
    for ref in sent:
        pltpu.make_async_copy(ref, ref, send_sem.at[0]).wait()


def write_kernel(
    val_ref, grad_ref, loss_ref, wt_ref, raw_ref, scaled_ref, coef_ref, lcol_ref,
    out_ref, gout_ref, lout_ref, buf, lbuf, sem,
):
    copies = []

    def put(src, i):
        c = pltpu.make_async_copy(src, out_ref.at[pl.ds(i * CB, CB)], sem.at[i])
        c.start()
        copies.append(c)

    for i in range(NK):
        put(val_ref.at[pl.ds(i * CB, CB)], i)
    lbuf[...] = loss_ref[0:1, 0:ROWS]
    copies.append(pltpu.make_async_copy(grad_ref, gout_ref, sem.at[NCB]))
    copies.append(pltpu.make_async_copy(lbuf, lout_ref, sem.at[NCB + 1]))
    for c in copies[NK:]:
        c.start()
    for i in range(NK, NCB):
        buf[i - NK] = class_rows(i, lcol_ref, coef_ref, wt_ref, raw_ref, scaled_ref)
        put(buf.at[i - NK], i)
    for c in copies:
        c.wait()


def whole(embeddings, labels, centers):
    vm = pl.BlockSpec(memory_space=pltpu.VMEM)
    hbm = pl.BlockSpec(memory_space=pltpu.HBM)
    made = pl.pallas_call(
        head_kernel,
        out_shape=(
            pltpu.VMEM((NK * CB, D), F32),
            pltpu.VMEM((ROWS, D), F32),
            pltpu.VMEM((1, 128), F32),
            pltpu.VMEM((C, B), BF16),
            pltpu.VMEM((C, D), BF16),
            pltpu.VMEM((B, D), BF16),
            pltpu.VMEM((8, B), F32),
            pltpu.VMEM((8, B), jnp.int32),
        ),
        in_specs=[hbm] * 3,
        out_specs=(vm,) * 8,
        scratch_shapes=[
            pltpu.SMEM((ROWS,), jnp.int32),
            pltpu.VMEM((ROWS, D), BF16),
            pltpu.VMEM((NY, NX, NZ, ROWS, D), BF16),
            pltpu.VMEM((NY, NX, NZ, 1, 128), jnp.int32),
            pltpu.VMEM((C, D), BF16),
            pltpu.VMEM((D, C), BF16),
            pltpu.VMEM((B, D), BF16),
            pltpu.VMEM((2, CB, HB), F32),
            pltpu.VMEM((B, 128), F32),
            pltpu.VMEM((8, B), F32),
            pltpu.VMEM((2, 4, 128), F32),
            pltpu.VMEM((7, 4, 128), F32),
            pltpu.VMEM((7, 4, 128), F32),
            pltpu.VMEM((4, 128), F32),
            pltpu.VMEM((2, NX, 64, D), BF16),
            pltpu.VMEM((64, D), BF16),
            pltpu.VMEM((2, 2, 64, D), BF16),
            pltpu.VMEM((3, 64, D), BF16),
            pltpu.VMEM((2, 64, D), BF16),
            pltpu.VMEM((NZ, ROWS, D), BF16),
            pltpu.VMEM((7, ROWS, D), BF16),
            pltpu.VMEM((2, NX, 64, D), BF16),
            pltpu.VMEM((NX, 64, D), F32),
            pltpu.VMEM((2, 64, D), BF16),
            pltpu.VMEM((64, D), BF16),
            pltpu.VMEM((5, 64, D), BF16),
            pltpu.VMEM((NZ, ROWS, D), F32),
            pltpu.VMEM((NZ, ROWS, D), BF16),
            pltpu.VMEM((7, ROWS, D), BF16),
            pltpu.SemaphoreType.DMA((NCB + 2,)),
            pltpu.SemaphoreType.DMA((1,)),
            pltpu.SemaphoreType.DMA((38,)),
        ],
        compiler_params=pltpu.CompilerParams(
            collective_id=0, has_side_effects=True, vmem_limit_bytes=48 * 1024 * 1024
        ),
        name="head",
    )(labels, embeddings, centers)
    out, grad, loss = pl.pallas_call(
        write_kernel,
        out_shape=(
            jax.ShapeDtypeStruct((C, D), F32),
            jax.ShapeDtypeStruct((ROWS, D), F32),
            jax.ShapeDtypeStruct((1, ROWS), F32),
        ),
        in_specs=[vm] * 8,
        out_specs=(hbm,) * 3,
        scratch_shapes=[
            pltpu.VMEM((NCB - NK, CB, D), F32),
            pltpu.VMEM((1, ROWS), F32),
            pltpu.SemaphoreType.DMA((NCB + 2,)),
        ],
        compiler_params=pltpu.CompilerParams(vmem_limit_bytes=12 * 1024 * 1024),
        name="write",
    )(*made)
    return loss.reshape(ROWS), grad, out


def solution(mesh):
    in_specs = (P(("dp", "cls"), None), P(("dp", "cls")), P(("dp", "cls"), None))
    out_specs = (P(("dp", "cls")), P(("dp", "cls"), None), P(("dp", "cls"), None))
    return jax.shard_map(
        whole, mesh=mesh, in_specs=in_specs, out_specs=out_specs, check_vma=False
    )
```

```python
import functools
import math

import jax
import jax.numpy as jnp
from jax import lax
from jax.experimental import pallas as pl
from jax.experimental.pallas import tpu as pltpu
from jax.sharding import PartitionSpec as P

MC = math.cos(0.5)
MS = math.sin(0.5)
EPS = 1e-06
NX, NY, NZ = 4, 2, 8
ROWS = 8
D = 512
C = 4096
B = 512
CB = 512
NCB = C // CB
F32 = jnp.float32
BF16 = jnp.bfloat16
ZOFF = (0, 1, 7, 2, 6, 3, 5, 4)
XY = ((1, 0), (3, 0), (2, 0), (0, 1), (1, 1), (3, 1), (2, 1))
HB = B // 2
NK = 5
HALVES = (slice(0, D // 2), slice(D // 2, D))
LOG2E = 64.0 / math.log(2.0)


def pid(x, y, z):
    return x * (NY * NZ) + z * NY + y


def class_rows(i, lcol_ref, coef_ref, wt_ref, raw_ref, scaled_ref):
    rows = slice(i * CB, (i + 1) * CB)
    rid = lax.broadcasted_iota(jnp.int32, (CB, B), 0) + i * CB
    w = jnp.where(rid == lcol_ref[0:1], coef_ref[0:1], wt_ref[rows].astype(F32)).astype(BF16)
    g = jnp.dot(w, scaled_ref[...], preferred_element_type=F32)
    v = raw_ref[rows].astype(F32)
    inv = lax.rsqrt(jnp.sum(v * v, axis=1, keepdims=True) + EPS)
    dot = jnp.sum(v * g, axis=1, keepdims=True)
    return inv * g - (inv * inv * inv * dot) * v


def head_kernel(
    lab_hbm, emb_hbm, cen_ref,
    out_ref, grad_ref, loss_ref, wt_ref, raw_ref, scaled_ref, coef_ref, lcol_ref,
    lab_ref, emb_ref, xg, lg, hat, hat_t, ehat, cosb, lcolb, tacc,
    csend, crecv_xy, crecv_z, ctot,
    psend, precv_y, precv_x13, psum, precv_x, pz, precv_z,
    nsend, nown, nrecv_a, nmid, nrecv, nz, nz_b, nrecv_z,
    cen_sem, send_sem, recv_sem,
):
    me = lax.axis_index("cls")
    x = me // (NY * NZ)
    z = (me % (NY * NZ)) // NY
    y = me % NY
    ys = (y, 1 - y)
    xk = {k: (x + k) % NX for k in range(NX)}
    zpeers = [pid(x, y, (z + k) % NZ) for k in ZOFF[1:]]
    ypeer = pid(x, ys[1], z)
    xypeers = [pid(xk[k], ys[h], z) for k, h in XY]
    base = me * C

    barrier = pltpu.get_barrier_semaphore()
    for p in zpeers + xypeers:
        pl.semaphore_signal(barrier, inc=1, device_id={"cls": p})

    whole_cen = pltpu.make_async_copy(cen_ref, raw_ref, cen_sem.at[0])
    small = [
        pltpu.make_async_copy(lab_hbm, lab_ref, cen_sem.at[1]),
        pltpu.make_async_copy(emb_hbm, emb_ref, cen_sem.at[2]),
    ]
    for c in small:
        c.start()
    whole_cen.start()

    lane = lax.broadcasted_iota(jnp.int32, (1, 128), 1)
    off = (x % 2) * 64 + z * ROWS
    lrow = jnp.zeros((1, 128), jnp.int32)
    for c in small:
        c.wait()
    for r in range(ROWS):
        lrow = jnp.where(lane == off + r, lab_ref[r], lrow)
    lg[y, x, z] = lrow
    xg[y, x, z] = emb_ref[...]

    def norm_block(i):
        rows = pl.ds(i * CB, CB)
        v = raw_ref[rows].astype(F32)
        inv = lax.rsqrt(jnp.sum(v * v, axis=1, keepdims=True) + EPS)
        hat[rows] = (v * inv).astype(BF16)

    def turn_block(i):
        rows = pl.ds(i * CB, CB)
        hat_t[:, rows] = hat[rows].T

    def apart(body):
        pl.when(me >= 0)(body)

    pl.semaphore_wait(barrier, 14)

    groups = []
    sent = []

    def group():
        groups.append(None)
        return len(groups) - 1

    def go(src, dst, peer, g):
        pltpu.make_async_remote_copy(
            src_ref=src, dst_ref=dst, send_sem=send_sem.at[0], recv_sem=recv_sem.at[g],
            device_id={"cls": peer},
        ).start()

    def arrive(g, ref):
        pltpu.make_async_copy(ref, ref, recv_sem.at[g]).wait()
        sent.append(ref)

    lsl = lg.at[y, x, z]
    lz = group()
    for p in zpeers:
        go(lsl, lsl, p, lz)
    ez = [group() for p in zpeers]
    for g, p in reversed(list(zip(ez, zpeers))):
        go(emb_ref, xg.at[y, x, z], p, g)
    xf = [group() for j in range(NZ)]
    yf = [group() for j in range(NZ)]
    rest = group()

    def zat(j):
        return (z + NZ - ZOFF[j]) % NZ

    def forward_x(j):
        blk = xg.at[y, x, zat(j)]
        for k in (1, 3, 2):
            go(blk, blk, pid(xk[k], y, z), xf[j])

    def forward_y(k, j):
        blk = xg.at[y, (x + NX - k) % NX, zat(j)]
        go(blk, blk, ypeer, rest if k else yf[j])

    def on_y(j):
        arrive(yf[j], emb_ref)
        blk = xg.at[ys[1], x, zat(j)]
        for k in (1, 3):
            go(blk, blk, pid(xk[k], y, z), rest)

    forward_x(0)
    forward_y(0, 0)

    work = [functools.partial(norm_block, i) for i in range(NCB)]

    def do(n):
        for _ in range(min(n, len(work))):
            work.pop(0)()

    def on_z(j):
        arrive(ez[j - 1], emb_ref)
        forward_x(j)
        forward_y(0, j)

    def on_x(j):
        arrive(xf[j], xg.at[y, x, pl.ds(0, 3)])
        forward_y(2, j)

    whole_cen.wait()
    do(NCB)
    on_z(1)
    on_z(2)
    on_z(3)
    on_z(4)
    on_x(0)
    on_z(5)
    on_z(6)
    on_z(7)
    arrive(lz, lg.at[y, x, pl.ds(0, 7)])
    lxy = [group(), group()]
    for i, p in enumerate(xypeers):
        go(lg.at[y, x], lg.at[y, x], p, lxy[min(i // 3, 1)])
    for j in range(1, NZ):
        on_x(j)
        on_y(j - 1)
    on_y(NZ - 1)

    def lab_half(h):
        return [
            jnp.sum(lg[ys[h], 2 * p : 2 * p + 2].reshape(2 * NZ, 128), axis=0, keepdims=True)
            - base
            for p in range(2)
        ]

    arrive(lxy[0], lg.at[y, pl.ds(0, 3)])
    labs = lab_half(0)
    lcols = [jnp.concatenate(labs, axis=1)]

    arrive(lxy[1], lg.at[y])
    labs += lab_half(1)
    lcols.append(jnp.concatenate(labs[2:], axis=1))
    lcol = jnp.concatenate(labs, axis=1)
    owned = (lcol >= 0) & (lcol < C)
    for q in range(4):
        lcolb[q * 128 : (q + 1) * 128] = jnp.broadcast_to(labs[q].astype(F32), (128, 128)).T

    py2, px13, px = group(), group(), group()

    def take_y2():
        arrive(py2, precv_y)
        v = psend[0, xk[2]].astype(F32) + precv_y[...].astype(F32)
        psum[0] = v.astype(BF16)
        go(psum.at[0], precv_x.at[0], pid(xk[2], y, z), px)

    def take_x13():
        arrive(px13, precv_x13)
        v = [
            psend[h, x].astype(F32) + precv_x13[0, h].astype(F32) + precv_x13[1, h].astype(F32)
            for h in range(2)
        ]
        psum[1] = v[1].astype(BF16)
        go(psum.at[1], precv_x.at[1], ypeer, px)
        psum[2] = v[0].astype(BF16)

    def pick_labels():
        acc = jnp.zeros((B, D), F32)
        lanef = lax.broadcasted_iota(jnp.int32, (1, 128), 1).astype(F32)
        for i in range(NCB):
            hot = jnp.concatenate(
                [
                    jnp.where(lcolb[...] == lanef + float(i * CB + g * 128), 1.0, 0.0)
                    for g in range(CB // 128)
                ],
                axis=1,
            ).astype(BF16)
            acc = acc + jnp.dot(
                hot, hat[i * CB : (i + 1) * CB], preferred_element_type=F32
            )
            turn_block(i)
        psend[...] = acc.astype(BF16).reshape(2, NX, 64, D)

    apart(pick_labels)
    go(psend.at[1, xk[2]], precv_y, ypeer, py2)
    for i, k in enumerate((1, 3)):
        go(psend.at[:, xk[k]], precv_x13.at[i], pid(xk[k], y, z), px13)

    def emb_half(h):
        e = xg[ys[h]].astype(F32)
        inv = lax.rsqrt(jnp.sum(e * e, axis=-1, keepdims=True) + EPS)
        ehat[h * HB : (h + 1) * HB] = (e * inv).reshape(HB, D).astype(BF16)

    def cos_chunk(h):
        cols = slice(h * HB, (h + 1) * HB)
        lc = lcols[h]

        def score(i):
            cosb[i % 2] = lax.dot_general(
                hat[i * CB : (i + 1) * CB], ehat[cols],
                (((1,), (1,)), ((), ())), preferred_element_type=F32,
            )

        t_acc = jnp.zeros((8, HB), F32)
        score(0)
        for i in range(NCB):
            if i + 1 < NCB:
                score(i + 1)
            rid = lax.broadcasted_iota(jnp.int32, (CB, HB), 0)
            e = jnp.where(rid == lc - i * CB, 0.0, jnp.exp2(LOG2E * cosb[i % 2]))
            wt_ref[i * CB : (i + 1) * CB, cols] = e.astype(BF16)
            t_acc = t_acc + jnp.sum(e.reshape(CB // 8, 8, HB), axis=0)
        tacc[:, cols] = t_acc

    def n_chunk(h):
        cols = slice(h * HB, (h + 1) * HB)
        t = jnp.dot(hat_t[...], wt_ref[:, cols], preferred_element_type=F32)
        t = t.T.reshape(NX, 64, D)
        nsend[h] = t.astype(BF16)
        if h == 0:
            nown[...] = t

    emb_half(0)
    apart(lambda: cos_chunk(0))
    arrive(rest, xg.at[ys[1], pl.ds(0, 3)])
    emb_half(1)
    apart(lambda: cos_chunk(1))
    t_part = jnp.sum(tacc[...], axis=0, keepdims=True)
    a = lax.broadcasted_iota(jnp.int32, (HB, HB), 0)
    b = lax.broadcasted_iota(jnp.int32, (HB, HB), 1)
    tc = []
    for h in range(2):
        m = lax.dot_general(
            ehat[h * HB : (h + 1) * HB], psend[h].reshape(HB, D),
            (((1,), (1,)), ((), ())), preferred_element_type=F32,
        )
        tc.append(jnp.sum(jnp.where(a == b, m, 0.0), axis=0, keepdims=True))
    tcos = jnp.concatenate(tc, axis=1)
    tsin = jnp.sqrt(1.04 - tcos * tcos)
    shifted = tcos * MC - tsin * MS
    slope = jnp.where(owned, MC + MS * tcos / tsin, 0.0)
    et = jnp.where(owned, jnp.exp2(LOG2E * shifted), 0.0)
    t_part = t_part + et
    where_t = [ys[0] * 2, ys[0] * 2 + 1, ys[1] * 2, ys[1] * 2 + 1]
    for q in range(4):
        csend[0, pl.ds(where_t[q], 1)] = t_part[:, q * 128 : (q + 1) * 128]
    cxy = group()
    for i, p in enumerate(xypeers):
        go(csend.at[0], crecv_xy.at[i], p, cxy)
    take_y2()
    apart(lambda: n_chunk(1))
    na, nx = (group(), group()), group()
    for h, lanes in enumerate(HALVES):
        for i, k in enumerate((1, 3)):
            src = nsend.at[1, xk[k], :, lanes]
            go(src, nrecv_a.at[i, :, lanes], pid(xk[k], y, z), na[h])
    go(nsend.at[1, xk[2]], nrecv.at[0], pid(xk[2], ys[1], z), nx)
    take_x13()
    apart(lambda: n_chunk(0))
    for k in (2, 1, 3):
        go(nsend.at[0, xk[k]], nrecv.at[k], pid(xk[k], y, z), nx)
    arrive(cxy, crecv_xy)
    tot = csend[0]
    for i in range(7):
        tot = tot + crecv_xy[i]
    csend[1] = tot
    cz = group()
    for i, p in reversed(list(enumerate(zpeers))):
        go(csend.at[1], crecv_z.at[i], p, cz)
    for h, lanes in enumerate(HALVES):
        arrive(na[h], nrecv_a.at[:, :, lanes])
        v = nsend[1, x, :, lanes].astype(F32)
        v = v + nrecv_a[0, :, lanes].astype(F32) + nrecv_a[1, :, lanes].astype(F32)
        nmid[:, lanes] = v.astype(BF16)
        go(nmid.at[:, lanes], nrecv.at[4, :, lanes], ypeer, nx)
    arrive(px, precv_x)
    s = psum[2].astype(F32) + precv_x[0].astype(F32) + precv_x[1].astype(F32)
    pz[...] = s.astype(BF16).reshape(NZ, ROWS, D)
    pzc = group()
    for i, (k, p) in reversed(list(enumerate(zip(ZOFF[1:], zpeers)))):
        go(pz.at[(z + k) % NZ], precv_z.at[i], p, pzc)
    arrive(nx, nrecv)
    s = nown[x]
    for i in range(5):
        s = s + nrecv[i].astype(F32)
    s = s.reshape(NZ, ROWS, D)
    nz[...] = s
    nz_b[...] = s.astype(BF16)
    nzc = group()
    for i, (k, p) in reversed(list(enumerate(zip(ZOFF[1:], zpeers)))):
        go(nz_b.at[(z + k) % NZ], nrecv_z.at[i], p, nzc)
    arrive(cz, crecv_z)
    tot = csend[1]
    for i in range(7):
        tot = tot + crecv_z[i]
    ctot[...] = tot

    total = jnp.concatenate([ctot[pl.ds(v, 1)] for v in where_t], axis=1)
    ca = 64.0 / total
    coef = slope * (et - total)
    for k in range(4):
        cols = slice(k * 128, (k + 1) * 128)
        col = jnp.broadcast_to(ca[:, cols], (128, 128)).T
        for j in range(4):
            dcols = slice(j * 128, (j + 1) * 128)
            v = ehat[cols, dcols].astype(F32) * col
            scaled_ref[cols, dcols] = v.astype(BF16)
    coef_ref[...] = jnp.broadcast_to(coef, (8, B))
    lcol_ref[...] = jnp.broadcast_to(lcol, (8, B))

    def class_block(i):
        out_ref[i * CB : (i + 1) * CB] = class_rows(
            i, lcol_ref, coef_ref, wt_ref, raw_ref, scaled_ref
        )

    for i in range(NK):
        apart(functools.partial(class_block, i))
    arrive(pzc, precv_z)
    pick = pz[z].astype(F32)
    for i in range(7):
        pick = pick + precv_z[i].astype(F32)
    e = emb_ref[...].astype(F32)
    inv = lax.rsqrt(jnp.sum(e * e, axis=1, keepdims=True) + EPS)
    u = e * inv
    tc = jnp.sum(u.astype(BF16).astype(F32) * pick, axis=1, keepdims=True)
    ts = jnp.sqrt(1.04 - tc * tc)
    sh = tc * MC - ts * MS
    sl = MC + MS * tc / ts
    sub = lax.broadcasted_iota(jnp.int32, (ROWS, 128), 0)
    lan = lax.broadcasted_iota(jnp.int32, (ROWS, 128), 1)
    trow = jnp.broadcast_to(ctot[pl.ds(y * 2 + x // 2, 1)], (ROWS, 128))
    tcol = jnp.sum(jnp.where(lan == sub + off, trow, 0.0), axis=1, keepdims=True)
    loss = jnp.log(tcol) - 64.0 * sh
    loss_ref[...] = jnp.sum(jnp.where(lan == sub, loss, 0.0), axis=0, keepdims=True)
    inv_t = 64.0 / tcol
    part = (sl * (jnp.exp2(LOG2E * sh) * inv_t - 64.0)) * pick
    arrive(nzc, nrecv_z)
    n = nz[z]
    for i in range(7):
        n = n + nrecv_z[i].astype(F32)
    g = n * inv_t + part
    grad_ref[...] = inv * (g - u * jnp.sum(u * g, axis=1, keepdims=True))
    for ref in sent:
        pltpu.make_async_copy(ref, ref, send_sem.at[0]).wait()


def write_kernel(
    val_ref, grad_ref, loss_ref, wt_ref, raw_ref, scaled_ref, coef_ref, lcol_ref,
    out_ref, gout_ref, lout_ref, buf, lbuf, sem,
):
    copies = []

    def put(src, i):
        c = pltpu.make_async_copy(src, out_ref.at[pl.ds(i * CB, CB)], sem.at[i])
        c.start()
        copies.append(c)

    for i in range(NK):
        put(val_ref.at[pl.ds(i * CB, CB)], i)
    lbuf[...] = loss_ref[0:1, 0:ROWS]
    copies.append(pltpu.make_async_copy(grad_ref, gout_ref, sem.at[NCB]))
    copies.append(pltpu.make_async_copy(lbuf, lout_ref, sem.at[NCB + 1]))
    for c in copies[NK:]:
        c.start()
    for i in range(NK, NCB):
        buf[i - NK] = class_rows(i, lcol_ref, coef_ref, wt_ref, raw_ref, scaled_ref)
        put(buf.at[i - NK], i)
    for c in copies:
        c.wait()


def whole(embeddings, labels, centers):
    vm = pl.BlockSpec(memory_space=pltpu.VMEM)
    hbm = pl.BlockSpec(memory_space=pltpu.HBM)
    made = pl.pallas_call(
        head_kernel,
        out_shape=(
            pltpu.VMEM((NK * CB, D), F32),
            pltpu.VMEM((ROWS, D), F32),
            pltpu.VMEM((1, 128), F32),
            pltpu.VMEM((C, B), BF16),
            pltpu.VMEM((C, D), BF16),
            pltpu.VMEM((B, D), BF16),
            pltpu.VMEM((8, B), F32),
            pltpu.VMEM((8, B), jnp.int32),
        ),
        in_specs=[hbm] * 3,
        out_specs=(vm,) * 8,
        scratch_shapes=[
            pltpu.SMEM((ROWS,), jnp.int32),
            pltpu.VMEM((ROWS, D), BF16),
            pltpu.VMEM((NY, NX, NZ, ROWS, D), BF16),
            pltpu.VMEM((NY, NX, NZ, 1, 128), jnp.int32),
            pltpu.VMEM((C, D), BF16),
            pltpu.VMEM((D, C), BF16),
            pltpu.VMEM((B, D), BF16),
            pltpu.VMEM((2, CB, HB), F32),
            pltpu.VMEM((B, 128), F32),
            pltpu.VMEM((8, B), F32),
            pltpu.VMEM((2, 4, 128), F32),
            pltpu.VMEM((7, 4, 128), F32),
            pltpu.VMEM((7, 4, 128), F32),
            pltpu.VMEM((4, 128), F32),
            pltpu.VMEM((2, NX, 64, D), BF16),
            pltpu.VMEM((64, D), BF16),
            pltpu.VMEM((2, 2, 64, D), BF16),
            pltpu.VMEM((3, 64, D), BF16),
            pltpu.VMEM((2, 64, D), BF16),
            pltpu.VMEM((NZ, ROWS, D), BF16),
            pltpu.VMEM((7, ROWS, D), BF16),
            pltpu.VMEM((2, NX, 64, D), BF16),
            pltpu.VMEM((NX, 64, D), F32),
            pltpu.VMEM((2, 64, D), BF16),
            pltpu.VMEM((64, D), BF16),
            pltpu.VMEM((5, 64, D), BF16),
            pltpu.VMEM((NZ, ROWS, D), F32),
            pltpu.VMEM((NZ, ROWS, D), BF16),
            pltpu.VMEM((7, ROWS, D), BF16),
            pltpu.SemaphoreType.DMA((3,)),
            pltpu.SemaphoreType.DMA((1,)),
            pltpu.SemaphoreType.DMA((38,)),
        ],
        compiler_params=pltpu.CompilerParams(
            collective_id=0, has_side_effects=True, vmem_limit_bytes=48 * 1024 * 1024
        ),
        name="head",
    )(labels, embeddings, centers)
    out, grad, loss = pl.pallas_call(
        write_kernel,
        out_shape=(
            jax.ShapeDtypeStruct((C, D), F32),
            jax.ShapeDtypeStruct((ROWS, D), F32),
            jax.ShapeDtypeStruct((1, ROWS), F32),
        ),
        in_specs=[vm] * 8,
        out_specs=(hbm,) * 3,
        scratch_shapes=[
            pltpu.VMEM((NCB - NK, CB, D), F32),
            pltpu.VMEM((1, ROWS), F32),
            pltpu.SemaphoreType.DMA((NCB + 2,)),
        ],
        compiler_params=pltpu.CompilerParams(vmem_limit_bytes=12 * 1024 * 1024),
        name="write",
    )(*made)
    return loss.reshape(ROWS), grad, out


def solution(mesh):
    in_specs = (P(("dp", "cls"), None), P(("dp", "cls")), P(("dp", "cls"), None))
    out_specs = (P(("dp", "cls")), P(("dp", "cls"), None), P(("dp", "cls"), None))
    return jax.shard_map(
        whole, mesh=mesh, in_specs=in_specs, out_specs=out_specs, check_vma=False
    )
```

```python
import functools
import math

import jax
import jax.numpy as jnp
from jax import lax
from jax.experimental import pallas as pl
from jax.experimental.pallas import tpu as pltpu
from jax.sharding import PartitionSpec as P

MC = math.cos(0.5)
MS = math.sin(0.5)
EPS = 1e-06
NX, NY, NZ = 4, 2, 8
ROWS = 8
D = 512
C = 4096
B = 512
CB = 512
NCB = C // CB
F32 = jnp.float32
BF16 = jnp.bfloat16
ZOFF = (0, 1, 7, 2, 6, 3, 5, 4)
XY = ((1, 0), (3, 0), (2, 0), (0, 1), (1, 1), (3, 1), (2, 1))
HB = B // 2
NK = 5
HALVES = tuple(slice(i * 128, (i + 1) * 128) for i in range(4))
LOG2E = 64.0 / math.log(2.0)


def pid(x, y, z):
    return x * (NY * NZ) + z * NY + y


def class_rows(i, lcol_ref, coef_ref, wt_ref, raw_ref, scaled_ref):
    rows = slice(i * CB, (i + 1) * CB)
    rid = lax.broadcasted_iota(jnp.int32, (CB, B), 0) + i * CB
    w = jnp.where(rid == lcol_ref[0:1], coef_ref[0:1], wt_ref[rows].astype(F32)).astype(BF16)
    g = jnp.dot(w, scaled_ref[...], preferred_element_type=F32)
    v = raw_ref[rows].astype(F32)
    inv = lax.rsqrt(jnp.sum(v * v, axis=1, keepdims=True) + EPS)
    dot = jnp.sum(v * g, axis=1, keepdims=True)
    return inv * g - (inv * inv * inv * dot) * v


def head_kernel(
    lab_hbm, emb_hbm, cen_ref,
    out_ref, grad_ref, loss_ref, wt_ref, raw_ref, scaled_ref, coef_ref, lcol_ref,
    lab_ref, emb_ref, xg, lg, hat, hat_t, ehat, cosb, lcolb, tacc,
    csend, crecv_xy, crecv_z, ctot,
    psend, precv_y, precv_x13, psum, precv_x, pz, precv_z,
    nsend, nown, nrecv_a, nmid, nrecv, nz, nz_b, nrecv_z,
    cen_sem, send_sem, recv_sem,
):
    me = lax.axis_index("cls")
    x = me // (NY * NZ)
    z = (me % (NY * NZ)) // NY
    y = me % NY
    ys = (y, 1 - y)
    xk = {k: (x + k) % NX for k in range(NX)}
    zpeers = [pid(x, y, (z + k) % NZ) for k in ZOFF[1:]]
    ypeer = pid(x, ys[1], z)
    xypeers = [pid(xk[k], ys[h], z) for k, h in XY]
    base = me * C

    barrier = pltpu.get_barrier_semaphore()
    for p in zpeers + xypeers:
        pl.semaphore_signal(barrier, inc=1, device_id={"cls": p})

    whole_cen = pltpu.make_async_copy(cen_ref, raw_ref, cen_sem.at[0])
    small = [
        pltpu.make_async_copy(lab_hbm, lab_ref, cen_sem.at[1]),
        pltpu.make_async_copy(emb_hbm, emb_ref, cen_sem.at[2]),
    ]
    for c in small:
        c.start()
    whole_cen.start()

    lane = lax.broadcasted_iota(jnp.int32, (1, 128), 1)
    off = (x % 2) * 64 + z * ROWS
    lrow = jnp.zeros((1, 128), jnp.int32)
    for c in small:
        c.wait()
    for r in range(ROWS):
        lrow = jnp.where(lane == off + r, lab_ref[r], lrow)
    lg[y, x, z] = lrow
    xg[y, x, z] = emb_ref[...]

    def norm_block(i):
        rows = pl.ds(i * CB, CB)
        v = raw_ref[rows].astype(F32)
        inv = lax.rsqrt(jnp.sum(v * v, axis=1, keepdims=True) + EPS)
        hat[rows] = (v * inv).astype(BF16)

    def turn_block(i):
        rows = pl.ds(i * CB, CB)
        hat_t[:, rows] = hat[rows].T

    def apart(body):
        pl.when(me >= 0)(body)

    pl.semaphore_wait(barrier, 14)

    groups = []
    sent = []

    def group():
        groups.append(None)
        return len(groups) - 1

    def go(src, dst, peer, g):
        pltpu.make_async_remote_copy(
            src_ref=src, dst_ref=dst, send_sem=send_sem.at[0], recv_sem=recv_sem.at[g],
            device_id={"cls": peer},
        ).start()

    def arrive(g, ref):
        pltpu.make_async_copy(ref, ref, recv_sem.at[g]).wait()
        sent.append(ref)

    lsl = lg.at[y, x, z]
    lz = group()
    for p in zpeers:
        go(lsl, lsl, p, lz)
    ez = [group() for p in zpeers]
    for g, p in reversed(list(zip(ez, zpeers))):
        go(emb_ref, xg.at[y, x, z], p, g)
    xf = [group() for j in range(NZ)]
    yf = [group() for j in range(NZ)]
    rest = group()

    def zat(j):
        return (z + NZ - ZOFF[j]) % NZ

    def forward_x(j):
        blk = xg.at[y, x, zat(j)]
        for k in (1, 3, 2):
            go(blk, blk, pid(xk[k], y, z), xf[j])

    def forward_y(k, j):
        blk = xg.at[y, (x + NX - k) % NX, zat(j)]
        go(blk, blk, ypeer, rest if k else yf[j])

    def on_y(j):
        arrive(yf[j], emb_ref)
        blk = xg.at[ys[1], x, zat(j)]
        for k in (1, 3):
            go(blk, blk, pid(xk[k], y, z), rest)

    forward_x(0)
    forward_y(0, 0)

    work = [functools.partial(norm_block, i) for i in range(NCB)]

    def do(n):
        for _ in range(min(n, len(work))):
            work.pop(0)()

    def on_z(j):
        arrive(ez[j - 1], emb_ref)
        forward_x(j)
        forward_y(0, j)

    def on_x(j):
        arrive(xf[j], xg.at[y, x, pl.ds(0, 3)])
        forward_y(2, j)

    whole_cen.wait()
    do(NCB)
    on_z(1)
    on_z(2)
    on_z(3)
    on_z(4)
    on_x(0)
    on_z(5)
    on_z(6)
    on_z(7)
    arrive(lz, lg.at[y, x, pl.ds(0, 7)])
    lxy = [group(), group()]
    for i, p in enumerate(xypeers):
        go(lg.at[y, x], lg.at[y, x], p, lxy[min(i // 3, 1)])
    for j in range(1, NZ):
        on_x(j)
        on_y(j - 1)
    on_y(NZ - 1)

    def lab_half(h):
        return [
            jnp.sum(lg[ys[h], 2 * p : 2 * p + 2].reshape(2 * NZ, 128), axis=0, keepdims=True)
            - base
            for p in range(2)
        ]

    arrive(lxy[0], lg.at[y, pl.ds(0, 3)])
    labs = lab_half(0)
    lcols = [jnp.concatenate(labs, axis=1)]

    arrive(lxy[1], lg.at[y])
    labs += lab_half(1)
    lcols.append(jnp.concatenate(labs[2:], axis=1))
    lcol = jnp.concatenate(labs, axis=1)
    owned = (lcol >= 0) & (lcol < C)
    for q in range(4):
        lcolb[q * 128 : (q + 1) * 128] = jnp.broadcast_to(labs[q].astype(F32), (128, 128)).T

    py2, px13, px = group(), group(), group()

    def take_y2():
        arrive(py2, precv_y)
        v = psend[0, xk[2]].astype(F32) + precv_y[...].astype(F32)
        psum[0] = v.astype(BF16)
        go(psum.at[0], precv_x.at[0], pid(xk[2], y, z), px)

    def take_x13():
        arrive(px13, precv_x13)
        v = [
            psend[h, x].astype(F32) + precv_x13[0, h].astype(F32) + precv_x13[1, h].astype(F32)
            for h in range(2)
        ]
        psum[1] = v[1].astype(BF16)
        go(psum.at[1], precv_x.at[1], ypeer, px)
        psum[2] = v[0].astype(BF16)

    def pick_labels():
        acc = jnp.zeros((B, D), F32)
        lanef = lax.broadcasted_iota(jnp.int32, (1, 128), 1).astype(F32)
        for i in range(NCB):
            hot = jnp.concatenate(
                [
                    jnp.where(lcolb[...] == lanef + float(i * CB + g * 128), 1.0, 0.0)
                    for g in range(CB // 128)
                ],
                axis=1,
            ).astype(BF16)
            acc = acc + jnp.dot(
                hot, hat[i * CB : (i + 1) * CB], preferred_element_type=F32
            )
            turn_block(i)
        psend[...] = acc.astype(BF16).reshape(2, NX, 64, D)

    apart(pick_labels)
    go(psend.at[1, xk[2]], precv_y, ypeer, py2)
    for i, k in enumerate((1, 3)):
        go(psend.at[:, xk[k]], precv_x13.at[i], pid(xk[k], y, z), px13)

    def emb_half(h):
        e = xg[ys[h]].astype(F32)
        inv = lax.rsqrt(jnp.sum(e * e, axis=-1, keepdims=True) + EPS)
        ehat[h * HB : (h + 1) * HB] = (e * inv).reshape(HB, D).astype(BF16)

    def cos_chunk(h):
        cols = slice(h * HB, (h + 1) * HB)
        lc = lcols[h]

        def score(i):
            cosb[i % 2] = lax.dot_general(
                hat[i * CB : (i + 1) * CB], ehat[cols],
                (((1,), (1,)), ((), ())), preferred_element_type=F32,
            )

        t_acc = jnp.zeros((8, HB), F32)
        score(0)
        for i in range(NCB):
            if i + 1 < NCB:
                score(i + 1)
            rid = lax.broadcasted_iota(jnp.int32, (CB, HB), 0)
            e = jnp.where(rid == lc - i * CB, 0.0, jnp.exp2(LOG2E * cosb[i % 2]))
            wt_ref[i * CB : (i + 1) * CB, cols] = e.astype(BF16)
            t_acc = t_acc + jnp.sum(e.reshape(CB // 8, 8, HB), axis=0)
        tacc[:, cols] = t_acc

    def n_chunk(h):
        cols = slice(h * HB, (h + 1) * HB)
        t = jnp.dot(hat_t[...], wt_ref[:, cols], preferred_element_type=F32)
        t = t.T.reshape(NX, 64, D)
        nsend[h] = t.astype(BF16)
        if h == 0:
            nown[...] = t

    emb_half(0)
    apart(lambda: cos_chunk(0))
    arrive(rest, xg.at[ys[1], pl.ds(0, 3)])
    emb_half(1)
    apart(lambda: cos_chunk(1))
    t_part = jnp.sum(tacc[...], axis=0, keepdims=True)
    a = lax.broadcasted_iota(jnp.int32, (HB, HB), 0)
    b = lax.broadcasted_iota(jnp.int32, (HB, HB), 1)
    tc = []
    for h in range(2):
        m = lax.dot_general(
            ehat[h * HB : (h + 1) * HB], psend[h].reshape(HB, D),
            (((1,), (1,)), ((), ())), preferred_element_type=F32,
        )
        tc.append(jnp.sum(jnp.where(a == b, m, 0.0), axis=0, keepdims=True))
    tcos = jnp.concatenate(tc, axis=1)
    tsin = jnp.sqrt(1.04 - tcos * tcos)
    shifted = tcos * MC - tsin * MS
    slope = jnp.where(owned, MC + MS * tcos / tsin, 0.0)
    et = jnp.where(owned, jnp.exp2(LOG2E * shifted), 0.0)
    t_part = t_part + et
    where_t = [ys[0] * 2, ys[0] * 2 + 1, ys[1] * 2, ys[1] * 2 + 1]
    for q in range(4):
        csend[0, pl.ds(where_t[q], 1)] = t_part[:, q * 128 : (q + 1) * 128]
    cxy = group()
    for i, p in enumerate(xypeers):
        go(csend.at[0], crecv_xy.at[i], p, cxy)
    take_y2()
    apart(lambda: n_chunk(1))
    na, nx = [group() for _ in HALVES], group()
    for h, lanes in enumerate(HALVES):
        for i, k in enumerate((1, 3)):
            src = nsend.at[1, xk[k], :, lanes]
            go(src, nrecv_a.at[i, :, lanes], pid(xk[k], y, z), na[h])
    go(nsend.at[1, xk[2]], nrecv.at[0], pid(xk[2], ys[1], z), nx)
    take_x13()
    apart(lambda: n_chunk(0))
    for k in (2, 1, 3):
        go(nsend.at[0, xk[k]], nrecv.at[k], pid(xk[k], y, z), nx)
    arrive(cxy, crecv_xy)
    tot = csend[0]
    for i in range(7):
        tot = tot + crecv_xy[i]
    csend[1] = tot
    cz = group()
    for i, p in reversed(list(enumerate(zpeers))):
        go(csend.at[1], crecv_z.at[i], p, cz)
    for h, lanes in enumerate(HALVES):
        arrive(na[h], nrecv_a.at[:, :, lanes])
        v = nsend[1, x, :, lanes].astype(F32)
        v = v + nrecv_a[0, :, lanes].astype(F32) + nrecv_a[1, :, lanes].astype(F32)
        nmid[:, lanes] = v.astype(BF16)
        go(nmid.at[:, lanes], nrecv.at[4, :, lanes], ypeer, nx)
    arrive(px, precv_x)
    s = psum[2].astype(F32) + precv_x[0].astype(F32) + precv_x[1].astype(F32)
    pz[...] = s.astype(BF16).reshape(NZ, ROWS, D)
    pzc = group()
    for i, (k, p) in reversed(list(enumerate(zip(ZOFF[1:], zpeers)))):
        go(pz.at[(z + k) % NZ], precv_z.at[i], p, pzc)
    arrive(nx, nrecv)
    s = nown[x]
    for i in range(5):
        s = s + nrecv[i].astype(F32)
    s = s.reshape(NZ, ROWS, D)
    nz[...] = s
    nz_b[...] = s.astype(BF16)
    nzc = group()
    for i, (k, p) in reversed(list(enumerate(zip(ZOFF[1:], zpeers)))):
        go(nz_b.at[(z + k) % NZ], nrecv_z.at[i], p, nzc)
    arrive(cz, crecv_z)
    tot = csend[1]
    for i in range(7):
        tot = tot + crecv_z[i]
    ctot[...] = tot

    total = jnp.concatenate([ctot[pl.ds(v, 1)] for v in where_t], axis=1)
    ca = 64.0 / total
    coef = slope * (et - total)
    for k in range(4):
        cols = slice(k * 128, (k + 1) * 128)
        col = jnp.broadcast_to(ca[:, cols], (128, 128)).T
        for j in range(4):
            dcols = slice(j * 128, (j + 1) * 128)
            v = ehat[cols, dcols].astype(F32) * col
            scaled_ref[cols, dcols] = v.astype(BF16)
    coef_ref[...] = jnp.broadcast_to(coef, (8, B))
    lcol_ref[...] = jnp.broadcast_to(lcol, (8, B))

    def class_block(i):
        out_ref[i * CB : (i + 1) * CB] = class_rows(
            i, lcol_ref, coef_ref, wt_ref, raw_ref, scaled_ref
        )

    for i in range(NK):
        apart(functools.partial(class_block, i))
    arrive(pzc, precv_z)
    pick = pz[z].astype(F32)
    for i in range(7):
        pick = pick + precv_z[i].astype(F32)
    e = emb_ref[...].astype(F32)
    inv = lax.rsqrt(jnp.sum(e * e, axis=1, keepdims=True) + EPS)
    u = e * inv
    tc = jnp.sum(u.astype(BF16).astype(F32) * pick, axis=1, keepdims=True)
    ts = jnp.sqrt(1.04 - tc * tc)
    sh = tc * MC - ts * MS
    sl = MC + MS * tc / ts
    sub = lax.broadcasted_iota(jnp.int32, (ROWS, 128), 0)
    lan = lax.broadcasted_iota(jnp.int32, (ROWS, 128), 1)
    trow = jnp.broadcast_to(ctot[pl.ds(y * 2 + x // 2, 1)], (ROWS, 128))
    tcol = jnp.sum(jnp.where(lan == sub + off, trow, 0.0), axis=1, keepdims=True)
    loss = jnp.log(tcol) - 64.0 * sh
    loss_ref[...] = jnp.sum(jnp.where(lan == sub, loss, 0.0), axis=0, keepdims=True)
    inv_t = 64.0 / tcol
    part = (sl * (jnp.exp2(LOG2E * sh) * inv_t - 64.0)) * pick
    arrive(nzc, nrecv_z)
    n = nz[z]
    for i in range(7):
        n = n + nrecv_z[i].astype(F32)
    g = n * inv_t + part
    grad_ref[...] = inv * (g - u * jnp.sum(u * g, axis=1, keepdims=True))
    for ref in sent:
        pltpu.make_async_copy(ref, ref, send_sem.at[0]).wait()


def write_kernel(
    val_ref, grad_ref, loss_ref, wt_ref, raw_ref, scaled_ref, coef_ref, lcol_ref,
    out_ref, gout_ref, lout_ref, buf, lbuf, sem,
):
    copies = []

    def put(src, i):
        c = pltpu.make_async_copy(src, out_ref.at[pl.ds(i * CB, CB)], sem.at[i])
        c.start()
        copies.append(c)

    for i in range(NK):
        put(val_ref.at[pl.ds(i * CB, CB)], i)
    lbuf[...] = loss_ref[0:1, 0:ROWS]
    copies.append(pltpu.make_async_copy(grad_ref, gout_ref, sem.at[NCB]))
    copies.append(pltpu.make_async_copy(lbuf, lout_ref, sem.at[NCB + 1]))
    for c in copies[NK:]:
        c.start()
    for i in range(NK, NCB):
        buf[i - NK] = class_rows(i, lcol_ref, coef_ref, wt_ref, raw_ref, scaled_ref)
        put(buf.at[i - NK], i)
    for c in copies:
        c.wait()


def whole(embeddings, labels, centers):
    vm = pl.BlockSpec(memory_space=pltpu.VMEM)
    hbm = pl.BlockSpec(memory_space=pltpu.HBM)
    made = pl.pallas_call(
        head_kernel,
        out_shape=(
            pltpu.VMEM((NK * CB, D), F32),
            pltpu.VMEM((ROWS, D), F32),
            pltpu.VMEM((1, 128), F32),
            pltpu.VMEM((C, B), BF16),
            pltpu.VMEM((C, D), BF16),
            pltpu.VMEM((B, D), BF16),
            pltpu.VMEM((8, B), F32),
            pltpu.VMEM((8, B), jnp.int32),
        ),
        in_specs=[hbm] * 3,
        out_specs=(vm,) * 8,
        scratch_shapes=[
            pltpu.SMEM((ROWS,), jnp.int32),
            pltpu.VMEM((ROWS, D), BF16),
            pltpu.VMEM((NY, NX, NZ, ROWS, D), BF16),
            pltpu.VMEM((NY, NX, NZ, 1, 128), jnp.int32),
            pltpu.VMEM((C, D), BF16),
            pltpu.VMEM((D, C), BF16),
            pltpu.VMEM((B, D), BF16),
            pltpu.VMEM((2, CB, HB), F32),
            pltpu.VMEM((B, 128), F32),
            pltpu.VMEM((8, B), F32),
            pltpu.VMEM((2, 4, 128), F32),
            pltpu.VMEM((7, 4, 128), F32),
            pltpu.VMEM((7, 4, 128), F32),
            pltpu.VMEM((4, 128), F32),
            pltpu.VMEM((2, NX, 64, D), BF16),
            pltpu.VMEM((64, D), BF16),
            pltpu.VMEM((2, 2, 64, D), BF16),
            pltpu.VMEM((3, 64, D), BF16),
            pltpu.VMEM((2, 64, D), BF16),
            pltpu.VMEM((NZ, ROWS, D), BF16),
            pltpu.VMEM((7, ROWS, D), BF16),
            pltpu.VMEM((2, NX, 64, D), BF16),
            pltpu.VMEM((NX, 64, D), F32),
            pltpu.VMEM((2, 64, D), BF16),
            pltpu.VMEM((64, D), BF16),
            pltpu.VMEM((5, 64, D), BF16),
            pltpu.VMEM((NZ, ROWS, D), F32),
            pltpu.VMEM((NZ, ROWS, D), BF16),
            pltpu.VMEM((7, ROWS, D), BF16),
            pltpu.SemaphoreType.DMA((3,)),
            pltpu.SemaphoreType.DMA((1,)),
            pltpu.SemaphoreType.DMA((40,)),
        ],
        compiler_params=pltpu.CompilerParams(
            collective_id=0, has_side_effects=True, vmem_limit_bytes=48 * 1024 * 1024
        ),
        name="head",
    )(labels, embeddings, centers)
    out, grad, loss = pl.pallas_call(
        write_kernel,
        out_shape=(
            jax.ShapeDtypeStruct((C, D), F32),
            jax.ShapeDtypeStruct((ROWS, D), F32),
            jax.ShapeDtypeStruct((1, ROWS), F32),
        ),
        in_specs=[vm] * 8,
        out_specs=(hbm,) * 3,
        scratch_shapes=[
            pltpu.VMEM((NCB - NK, CB, D), F32),
            pltpu.VMEM((1, ROWS), F32),
            pltpu.SemaphoreType.DMA((NCB + 2,)),
        ],
        compiler_params=pltpu.CompilerParams(vmem_limit_bytes=12 * 1024 * 1024),
        name="write",
    )(*made)
    return loss.reshape(ROWS), grad, out


def solution(mesh):
    in_specs = (P(("dp", "cls"), None), P(("dp", "cls")), P(("dp", "cls"), None))
    out_specs = (P(("dp", "cls")), P(("dp", "cls"), None), P(("dp", "cls"), None))
    return jax.shard_map(
        whole, mesh=mesh, in_specs=in_specs, out_specs=out_specs, check_vma=False
    )
```
